256 devices in a mesh: grp: 4 (over x), wide: 64 (over y, z, core).
Axes of the slice: x: 4, y: 4, z: 8, core: 2. Of those that a mesh axis runs over, the one named last changes fastest.
Arguments:
- leaf_entries: float32 [4, 128, 512, 512], P('grp', 'wide'), may hold values from -8 to 14, as said below
- leaf_tiles: int32 [4, 128], P('grp', 'wide'), may hold values from 1 to 3
- leaf_map: int32 [4, 128, 3], P('grp', 'wide'), may hold values from 0 to 7, as said below
- mid_entries: float32 [4, 64, 1024, 1024], P('grp', 'wide'), may hold values from -8 to 14, as said below
- mid_tiles: int32 [4, 64], P('grp', 'wide'), may hold values from 3 to 7, as said below
- mid_map: int32 [4, 64, 7], P('grp', 'wide'), may hold values from 0 to 55, as said below
- root_panel_entries: float32 [4, 7680, 512], P('grp', 'wide'), may hold values from -8 to 14, as said below
- root_update_entries: float32 [4, 64, 896, 896], P('grp', 'wide'), may hold values from -1 to 5, as said below
Outputs:
- root_panel: float32 [4, 7680, 512], P('grp', 'wide')
- top_update: float32 [64, 896, 896], P('wide', 'grp')
The draws below stay inside these ranges and needn't reach their ends.
Inputs may be any that keep to these rules, and one draw needn't show every extreme that they name: `mid_tiles`: each group has a middle front with 7 live update tiles. `leaf_map`: the 3 entries of one leaf are distinct and less than 1 + mid_tiles of its middle front. `mid_map`: entry a of a middle front lies in the block (s + a) mod 8 of 7 consecutive tiles, s a multiple of 1 chosen for each front; so the live tiles of one middle update that land in one block of step four number at most 1, and in every draw some middle update sends exactly 1 to one block. `leaf_entries`: each leaf front is symmetric positive definite. `mid_entries`: each middle front is symmetric positive definite. `root_panel_entries`: the first 512 rows form a symmetric positive definite block. `root_update_entries`: the assembled square of step four before the additions is symmetric.
All inputs are finite; a program needn't handle non-finite values.
Results may differ from the reference program's by a relative error of at most 0.0003.
Values sent between devices are 32-bit elements; how exact they have to be, the bound alone decides.
No kernel may reach another device: no remote copies, remote signals or barrier semaphores. Data moves between devices by JAX's collectives and lax.ppermute only.
A program may use at most 128 MiB of HBM per device.

```python
import jax
import jax.numpy as jnp
from jax import lax

TILE = 128
LEAF_DEV = 2
UL = 3
FL = 4
UM = 7
FM = 8
K = 4
UT = 56
R = 60
LEAVES = 128
PCOL = 8
UR = 7
UC = 7
N_GRP = 4
N_WIDE = 64


def unit_matrix(key, order_rows):
    noise = jax.random.normal(key, (order_rows, order_rows), jnp.float32)
    symmetric = (noise + noise.T) * (0.3 / jnp.sqrt(2.0 * order_rows))
    return jnp.eye(order_rows, dtype=jnp.float32) + symmetric


def row_scales(key, order_rows):
    return jnp.exp(jax.random.uniform(key, (order_rows,), jnp.float32, -0.6931472, 0.6931472))


def spread_matrix(key, order_rows, block_rows):
    width = block_rows * 5 // 4
    groups = order_rows // block_rows
    total_cols = groups * width
    noise = jax.random.truncated_normal(key, -3.0, 3.0, (order_rows, total_cols), jnp.float32)
    row_group = jnp.arange(order_rows, dtype=jnp.int32) // block_rows
    column_group = jnp.arange(total_cols, dtype=jnp.int32) // width
    weight_mask = jnp.where(row_group[:, None] == column_group[None, :], 1.0, 0.1)
    factor_rows = noise * weight_mask / jnp.sqrt(jnp.float32(width))
    product = jnp.dot(factor_rows, factor_rows.T, precision=lax.Precision.HIGHEST)
    return 0.5 * (product + product.T) + 0.02 * jnp.eye(order_rows, dtype=jnp.float32)


def dominant_matrix(key, order_rows):
    weight_key, scale_key = jax.random.split(key)
    inner = unit_matrix(weight_key, order_rows)
    root_scale = jnp.sqrt(row_scales(scale_key, order_rows))
    return inner * root_scale[:, None] * root_scale[None, :]


def coupled_front(key, order_rows):
    pivot_key, couple_key, trail_key, scale_key = jax.random.split(key, 4)
    rest_rows = order_rows - TILE
    pivot_block = spread_matrix(pivot_key, TILE, TILE)
    trail_block = unit_matrix(trail_key, rest_rows)
    spread = 0.5 * TILE ** (-0.5)
    coupling = jax.random.normal(couple_key, (rest_rows, TILE), jnp.float32) * spread
    pivot_factor = jnp.linalg.cholesky(pivot_block)
    lower_left = jnp.dot(coupling, pivot_factor.T, precision=lax.Precision.HIGHEST)
    product = jnp.dot(coupling, coupling.T, precision=lax.Precision.HIGHEST)
    lower_right = trail_block + 0.5 * (product + product.T)
    upper_half = jnp.concatenate([pivot_block, lower_left.T], axis=1)
    lower_half = jnp.concatenate([lower_left, lower_right], axis=1)
    whole_matrix = jnp.concatenate([upper_half, lower_half], axis=0)
    root_scale = jnp.sqrt(row_scales(scale_key, order_rows))
    return whole_matrix * root_scale[:, None] * root_scale[None, :]


def coupled_batch(key, count, order_rows):

    def draw_single(index):
        return coupled_front(jax.random.fold_in(key, index), order_rows)
    return lax.map(draw_single, jnp.arange(count, dtype=jnp.int32))


def draw_leaf_entries(key, part):
    batch = coupled_batch(jax.random.fold_in(key, 101), N_GRP * LEAVES, FL * TILE)
    return batch.reshape(N_GRP, LEAVES, FL * TILE, FL * TILE)


def draw_mid_entries(key, part):
    batch = coupled_batch(jax.random.fold_in(key, 102), N_GRP * N_WIDE, FM * TILE)
    return batch.reshape(N_GRP, N_WIDE, FM * TILE, FM * TILE)


def middle_live(key):
    live_count = jax.random.randint(jax.random.fold_in(key, 201), (N_GRP, N_WIDE), UL, UM + 1, dtype=jnp.int32)
    chosen = jax.random.randint(jax.random.fold_in(key, 202), (N_GRP, 1), 0, N_WIDE, dtype=jnp.int32)
    filled = jnp.arange(N_WIDE, dtype=jnp.int32)[None, :] == chosen
    return jnp.where(filled, UM, live_count).astype(jnp.int32)


def draw_mid_tiles(key, part):
    return middle_live(key)


def draw_leaf_map(key, part):
    live_count = middle_live(key)
    parent_live = jnp.repeat(live_count, LEAF_DEV, axis=1)
    scores = jax.random.randint(jax.random.fold_in(key, 203), (N_GRP, LEAVES, FM), 0, 1 << 20, dtype=jnp.int32)
    positions = jnp.arange(FM, dtype=jnp.int32)
    scores = scores * FM + positions[None, None, :]
    scores = scores + jnp.where(positions[None, None, :] >= 1 + parent_live[:, :, None], 1 << 26, 0)
    ranking = jnp.argsort(scores, axis=-1, stable=True)
    return ranking[:, :, :UL].astype(jnp.int32)


def draw_mid_map(key, part):
    group_width = 8 // PCOL
    starts = jax.random.randint(jax.random.fold_in(key, 301), (N_GRP, N_WIDE, 1), 0, 8 // group_width, dtype=jnp.int32) * group_width
    block_ids = (starts + jnp.arange(UM, dtype=jnp.int32)[None, None, :]) % 8
    offsets = jax.random.randint(jax.random.fold_in(key, 302), (N_GRP, N_WIDE, UM), 0, UR, dtype=jnp.int32)
    return (block_ids * UR + offsets).astype(jnp.int32)


def draw_root_panel_entries(key, part):

    def draw_group(index):
        group_key = jax.random.fold_in(jax.random.fold_in(key, 401), index)
        pivot_key = jax.random.fold_in(group_key, 0)
        couple_key = jax.random.fold_in(group_key, 1)
        pivot_scale_key = jax.random.fold_in(group_key, 3)
        pivot_inner = spread_matrix(pivot_key, K * TILE, TILE)
        pivot_scale = jnp.sqrt(row_scales(pivot_scale_key, K * TILE))
        pivot_block = pivot_inner * pivot_scale[:, None] * pivot_scale[None, :]
        coupling = jax.random.normal(couple_key, (UT * TILE, K * TILE), jnp.float32) * 0.02
        return jnp.concatenate([pivot_block, coupling], axis=0)
    return lax.map(draw_group, jnp.arange(N_GRP, dtype=jnp.int32))


def draw_root_update_entries(key, part):

    def draw_group(index):
        whole_matrix = dominant_matrix(jax.random.fold_in(jax.random.fold_in(key, 501), index), UT * TILE)
        block_view = whole_matrix.reshape(8, UR * TILE, PCOL, UC * TILE).transpose(0, 2, 1, 3)
        return block_view.reshape(N_WIDE, UR * TILE, UC * TILE)
    return lax.map(draw_group, jnp.arange(N_GRP, dtype=jnp.int32))


def touch_ends(values, rng, low, top_value):
    index_at = [jax.random.randint(jax.random.fold_in(rng, axis), (), 0, length) for axis, length in enumerate(values.shape)]
    widest = values.shape.index(max(values.shape))
    neighbour = index_at[:widest] + [(index_at[widest] + 1) % values.shape[widest]] + index_at[widest + 1:]
    return values.at[tuple(index_at)].set(low).at[tuple(neighbour)].set(top_value)


def setup_inputs(seed: int = 0) -> dict:
    keys = jax.random.split(jax.random.key(seed), 9)
    leaf_entries = draw_leaf_entries(jax.random.fold_in(keys[8], 71), 0)
    leaf_tiles = touch_ends(jax.random.randint(keys[1], (N_GRP, LEAVES), 1, UL + 1), jax.random.fold_in(keys[1], 1), 1, UL).astype(jnp.int32)
    leaf_map = draw_leaf_map(jax.random.fold_in(keys[8], 71), 0)
    mid_entries = draw_mid_entries(jax.random.fold_in(keys[8], 71), 0)
    mid_tiles = draw_mid_tiles(jax.random.fold_in(keys[8], 71), 0)
    mid_map = draw_mid_map(jax.random.fold_in(keys[8], 71), 0)
    root_panel_entries = draw_root_panel_entries(jax.random.fold_in(keys[8], 71), 0)
    root_update_entries = draw_root_update_entries(jax.random.fold_in(keys[8], 71), 0)
    return dict(leaf_entries=leaf_entries, leaf_tiles=leaf_tiles, leaf_map=leaf_map, mid_entries=mid_entries, mid_tiles=mid_tiles, mid_map=mid_map, root_panel_entries=root_panel_entries, root_update_entries=root_update_entries)


def partial_factor(front_mat, live_tiles):
    order_rows = front_mat.shape[0]
    tile_index = jnp.arange(order_rows, dtype=jnp.int32) // TILE
    live_rows = (tile_index < 1 + live_tiles).astype(jnp.float32)
    masked = front_mat * live_rows[:, None] * live_rows[None, :]
    pivot_factor = jnp.linalg.cholesky(masked[:TILE, :TILE])
    coupling = jax.scipy.linalg.solve_triangular(pivot_factor, masked[TILE:, :TILE].T, lower=True).T
    product = jnp.dot(coupling.astype(jnp.float32), coupling.T.astype(jnp.float32), precision=lax.Precision.HIGHEST, preferred_element_type=jnp.float32)
    return masked[TILE:, TILE:] - product

def middle_update(leaf_fronts, leaf_live, leaf_maps, middle_front, middle_count):
    leaf_updates = jax.vmap(partial_factor)(leaf_fronts, leaf_live)
    leaf_count = leaf_updates.shape[0]
    leaf_blocks = leaf_updates.reshape(leaf_count, UL, TILE, UL, TILE)
    onehot = (leaf_maps[:, None, :] == jnp.arange(FM, dtype=jnp.int32)[None, :, None]).astype(jnp.float32)
    spread = jnp.einsum('lpa,laxby->lpxby', onehot, leaf_blocks, precision=lax.Precision.HIGHEST)
    added = jnp.einsum('lpxby,lqb->pxqy', spread, onehot, precision=lax.Precision.HIGHEST)
    assembled = middle_front + added.reshape(FM * TILE, FM * TILE)
    return partial_factor(assembled, middle_count)

def reference(leaf_entries, leaf_tiles, leaf_map, mid_entries, mid_tiles, mid_map, root_panel_entries, root_update_entries):
    grid_cols = N_WIDE // 8
    row_tiles = UT // 8
    column_tiles = UT // grid_cols
    panels = []
    total = jnp.zeros((UT, UT, TILE, TILE), jnp.float32)
    all_tile = jnp.arange(R * TILE, dtype=jnp.int32) // TILE
    for group in range(N_GRP):
        leaf_fronts = leaf_entries[group].reshape(N_WIDE, LEAF_DEV, FL * TILE, FL * TILE)
        leaf_live = leaf_tiles[group].reshape(N_WIDE, LEAF_DEV)
        leaf_maps = leaf_map[group].reshape(N_WIDE, LEAF_DEV, UL)

        def one_middle(packed):
            return middle_update(packed[0], packed[1], packed[2], packed[3], packed[4])
        middle_updates = lax.map(one_middle, (leaf_fronts, leaf_live, leaf_maps, mid_entries[group], mid_tiles[group]))
        block_view = root_update_entries[group].reshape(8, grid_cols, row_tiles, TILE, column_tiles, TILE)
        update_tiles = block_view.transpose(0, 2, 1, 4, 3, 5).reshape(UT, UT, TILE, TILE)
        group_map = mid_map[group]

        def add_middle(index, current):
            pieces = middle_updates[index].reshape(UM, TILE, UM, TILE).transpose(0, 2, 1, 3)
            targets = group_map[index]
            return current.at[targets[:, None], targets[None, :]].add(pieces)
        update_tiles = lax.fori_loop(0, N_WIDE, add_middle, update_tiles)
        panel = root_panel_entries[group]
        columns = []
        for pivot in range(K):
            column = panel[:, pivot * TILE:(pivot + 1) * TILE]
            factor = jnp.linalg.cholesky(column[pivot * TILE:(pivot + 1) * TILE])
            solved = jax.scipy.linalg.solve_triangular(factor, column.T, lower=True).T
            solved = jnp.where(all_tile[:, None] > pivot, solved, 0.0)
            solved = solved.at[pivot * TILE:(pivot + 1) * TILE].set(factor)
            leading = jnp.where(all_tile[:K * TILE, None] > pivot, solved[:K * TILE], 0.0)
            panel = panel - jnp.dot(solved.astype(jnp.float32), leading.T.astype(jnp.float32), precision=lax.Precision.HIGHEST, preferred_element_type=jnp.float32)
            lower_rows = solved[K * TILE:].reshape(UT, TILE, TILE)
            update_tiles = update_tiles - jnp.einsum('axk,byk->abxy', lower_rows, lower_rows, precision=lax.Precision.HIGHEST)
            columns.append(solved)
        panels.append(jnp.concatenate(columns, axis=1))
        total = total + update_tiles
    top_view = total.reshape(8, row_tiles, grid_cols, column_tiles, TILE, TILE).transpose(0, 2, 1, 4, 3, 5)
    top_update = top_view.reshape(N_WIDE, row_tiles * TILE, column_tiles * TILE)
    return (jnp.stack(panels), top_update)
```

```python
import jax
import jax.numpy as jnp
from jax import lax
from jax.experimental import pallas as pl
from jax.experimental.pallas import tpu as pltpu
from jax.sharding import Mesh, PartitionSpec as P


TILE = 128
UL = 3
UM = 7
K = 4
BLK = 16
SLOT = 136
PANEL = 120
CHUNK = 112
SIDE = 896
HI = lax.Precision.HIGHEST
F32 = jnp.float32
COST = 1 << 31
WIDE = ("y", "h", "l", "c")


def dot(lhs, rhs, contract):
    return lax.dot_general(
        lhs, rhs, (contract, ((), ())), precision=HI, preferred_element_type=F32
    )


def factor_rows(panels):
    for block in range(TILE // BLK):
        low = block * BLK
        high = low + BLK
        work = []
        for ref, row, col, tiles in panels:
            rows = [
                ref[row + low : row + high, col + t * TILE : col + (t + 1) * TILE]
                for t in range(tiles)
            ]
            cols = [
                jnp.broadcast_to(rows[0][:, low + m : low + m + 1], (BLK, TILE))
                for m in range(BLK)
            ]
            work.append((rows, cols))
        for step in range(BLK):
            for (ref, row, col, tiles), (rows, cols) in zip(panels, work):
                inverse = lax.rsqrt(cols[step][step : step + 1, :])
                lower = cols[step] * inverse
                for t in range(tiles):
                    upper = rows[t][step : step + 1, :] * inverse
                    at = row + low + step
                    ref[at : at + 1, col + t * TILE : col + (t + 1) * TILE] = upper
                    if step + 1 < BLK:
                        rows[t] = rows[t] - lower * upper
                for m in range(step + 1, BLK):
                    cols[m] = cols[m] - lower * lower[m : m + 1, :]
        if high < TILE:
            for ref, row, col, tiles in panels:
                strip = ref[row + low : row + high, col : col + tiles * TILE]
                product = dot(strip[:, :TILE], strip, ((0,), (0,)))
                ref[row + high : row + TILE, col : col + tiles * TILE] = (
                    ref[row + high : row + TILE, col : col + tiles * TILE] - product[high:]
                )


def leaf_kernel(leaf_ref, out_ref, top):
    for i in range(2):
        top[i * TILE : (i + 1) * TILE, :] = leaf_ref[i, :TILE, :]
    factor_rows([(top, i * TILE, 0, UL + 1) for i in range(2)])
    for i in range(2):
        coupling = top[i * TILE : (i + 1) * TILE, TILE:]
        out_ref[i] = leaf_ref[i, TILE:, TILE:] - dot(coupling, coupling, ((0,), (0,)))


def leaves(leaf):
    return pl.pallas_call(
        leaf_kernel,
        out_shape=jax.ShapeDtypeStruct((2, UL * TILE, UL * TILE), F32),
        scratch_shapes=[pltpu.VMEM((2 * TILE, (UL + 1) * TILE), F32)],
        cost_estimate=pl.CostEstimate(flops=COST, bytes_accessed=3 << 20, transcendentals=0),
        name="leaves",
    )(leaf)


def middle_kernel(
    leaf_live, leaf_map, mid_live, mid_map, leaf_ref, mid_hbm, chunk_hbm, block_hbm, out_hbm,
    mid, update, spots, load_sem, send_sem, spot_sem,
):
    head = pltpu.make_async_copy(mid_hbm.at[:TILE], mid.at[:TILE], load_sem.at[0])
    rest = pltpu.make_async_copy(mid_hbm.at[TILE:], mid.at[TILE:], load_sem.at[1])
    head.start()
    rest.start()

    def assemble(in_head):
        for i in range(2):
            live = leaf_live[i]
            for a in range(UL):
                to_row = leaf_map[i * UL + a]
                row = pl.multiple_of(to_row * TILE, TILE)
                wanted = (to_row == 0) if in_head else (to_row > 0)
                for b in range(UL):
                    col = pl.multiple_of(leaf_map[i * UL + b] * TILE, TILE)

                    @pl.when(wanted & (a < live) & (b < live))
                    def _():
                        mid[pl.ds(row, TILE), pl.ds(col, TILE)] = (
                            mid[pl.ds(row, TILE), pl.ds(col, TILE)]
                            + leaf_ref[i, a * TILE : (a + 1) * TILE, b * TILE : (b + 1) * TILE]
                        )

    head.wait()
    assemble(True)
    factor_rows([(mid, 0, 0, UM + 1)])
    rest.wait()
    assemble(False)
    live = mid_live[0]
    spots[...] = jnp.zeros((64, SLOT - TILE, TILE), F32)
    copies = []
    for a in range(UM):
        update[a * TILE : (a + 1) * TILE, :] = mid[(a + 1) * TILE : (a + 2) * TILE, TILE:] - dot(
            mid[:TILE, (a + 1) * TILE : (a + 2) * TILE], mid[:TILE, TILE:], ((0,), (0,))
        )
        to_row = mid_map[a]
        for b in range(UM):
            to_col = mid_map[b]
            slot = (to_row // 7) * 8 + to_col // 7
            spot = (to_row % 7) * 7 + to_col % 7 + 1
            spot = jnp.where((a < live) & (b < live), spot, 0)
            spots[slot] = jnp.full((SLOT - TILE, TILE), spot.astype(F32), F32)
            copy = pltpu.make_async_copy(
                update.at[a * TILE : (a + 1) * TILE, b * TILE : (b + 1) * TILE],
                out_hbm.at[slot, :TILE, :],
                send_sem.at[a * UM + b],
            )
            copy.start()
            copies.append(copy)
    mark = pltpu.make_async_copy(spots, out_hbm.at[:, TILE:, :], spot_sem)
    mark.start()
    for copy in copies:
        copy.wait()
    mark.wait()


def middles(leaf_live, leaf_map, mid_live, mid_map, leaf, mid, chunk, block):
    smem = pl.BlockSpec(memory_space=pltpu.SMEM)
    vmem = pl.BlockSpec(memory_space=pltpu.VMEM)
    hbm = pl.BlockSpec(memory_space=pl.ANY)
    return pl.pallas_call(
        middle_kernel,
        out_shape=jax.ShapeDtypeStruct((64, SLOT, TILE), F32),
        in_specs=[smem, smem, smem, smem, vmem, hbm, hbm, hbm],
        out_specs=hbm,
        scratch_shapes=[
            pltpu.VMEM((1024, 1024), F32),
            pltpu.VMEM((SIDE, SIDE), F32),
            pltpu.VMEM((64, SLOT - TILE, TILE), F32),
            pltpu.SemaphoreType.DMA((2,)),
            pltpu.SemaphoreType.DMA((UM * UM,)),
            pltpu.SemaphoreType.DMA,
        ],
        cost_estimate=pl.CostEstimate(flops=COST, bytes_accessed=9 << 20, transcendentals=0),
        name="middles",
    )(leaf_live, leaf_map, mid_live, mid_map, leaf, mid, chunk, block)


def pivot_kernel(block_ref, inverse_ref, work):
    width = K * TILE
    eye = (
        lax.broadcasted_iota(jnp.int32, (width, width), 0)
        == lax.broadcasted_iota(jnp.int32, (width, width), 1)
    ).astype(F32)
    work[:, :width] = block_ref[...]
    work[:, width:] = eye
    for k in range(K):
        base = k * TILE
        end = width + base + TILE
        factor_rows([(work, base, base, K + 1)])
        for m in range(k + 1, K):
            off = m * TILE
            work[off : off + TILE, off:end] = work[off : off + TILE, off:end] - dot(
                work[base : base + TILE, off : off + TILE],
                work[base : base + TILE, off:end],
                ((0,), (0,)),
            )
    inverse_ref[...] = work[:, width:]


def pivots(block):
    width = K * TILE
    return pl.pallas_call(
        pivot_kernel,
        out_shape=jax.ShapeDtypeStruct((width, width), F32),
        scratch_shapes=[pltpu.VMEM((width, 2 * width), F32)],
        cost_estimate=pl.CostEstimate(flops=2 * COST, bytes_accessed=2 << 20, transcendentals=0),
        name="pivots",
    )(block)


def split(value):
    high = value.astype(jnp.bfloat16)
    return high, (value - high.astype(F32)).astype(jnp.bfloat16)


def update_kernel(
    first, row_ref, col_ref, own_ref, inverse_ref, entry_ref, panel_ref, out_ref, high, low
):
    width = K * TILE
    inverse = inverse_ref[...]
    rows_at = first[0] + lax.broadcasted_iota(jnp.int32, (PANEL, width), 0)
    column = lax.broadcasted_iota(jnp.int32, (PANEL, width), 1)
    live = (column <= rows_at) | (rows_at >= width)
    panel_ref[...] = jnp.where(live, dot(own_ref[...], inverse, ((1,), (1,))), 0.0)
    for side, ref in enumerate((row_ref, col_ref)):
        high[side], low[side] = split(dot(ref[...], inverse, ((1,), (1,))))

    def product(lhs, rhs):
        return lax.dot_general(
            lhs, rhs, (((1,), (1,)), ((), ())), preferred_element_type=F32
        )

    for t in range(7):
        at = slice(t * TILE, (t + 1) * TILE)
        out_ref[at, :] = entry_ref[at, :] - (
            product(high[0, at, :], high[1])
            + (product(high[0, at, :], low[1]) + product(low[0, at, :], high[1]))
        )


def updates(first, rows, cols, own, inverse, entries):
    vmem = pl.BlockSpec(memory_space=pltpu.VMEM)
    return pl.pallas_call(
        update_kernel,
        out_shape=(
            jax.ShapeDtypeStruct((PANEL, K * TILE), F32),
            jax.ShapeDtypeStruct((SIDE, SIDE), F32),
        ),
        in_specs=[pl.BlockSpec(memory_space=pltpu.SMEM)] + [vmem] * 5,
        out_specs=(vmem, vmem),
        scratch_shapes=[
            pltpu.VMEM((2, SIDE, K * TILE), jnp.bfloat16),
            pltpu.VMEM((2, SIDE, K * TILE), jnp.bfloat16),
        ],
        cost_estimate=pl.CostEstimate(flops=COST, bytes_accessed=12 << 20, transcendentals=0),
        name="updates",
    )(first, rows, cols, own, inverse, entries)


def place_kernel(incoming_hbm, base_ref, out_ref, incoming, spots, sem, spot_sem):
    parts = 4
    count = 64 // parts
    mark = pltpu.make_async_copy(incoming_hbm.at[:, TILE, :], spots, spot_sem)
    mark.start()
    copies = []
    for part in range(parts):
        at = pl.ds(part * count, count)
        copy = pltpu.make_async_copy(
            incoming_hbm.at[at, :TILE, :], incoming.at[at], sem.at[part]
        )
        copy.start()
        copies.append(copy)
    out_ref[...] = base_ref[...]
    mark.wait()
    for part, copy in enumerate(copies):
        copy.wait()

        def body(s, carry):
            spot = spots[s, 0].astype(jnp.int32)

            @pl.when(spot > 0)
            def _():
                row = pl.multiple_of(((spot - 1) // 7) * TILE, TILE)
                col = pl.multiple_of(((spot - 1) % 7) * TILE, TILE)
                out_ref[pl.ds(row, TILE), pl.ds(col, TILE)] = (
                    out_ref[pl.ds(row, TILE), pl.ds(col, TILE)] + incoming[s]
                )

            return carry

        lax.fori_loop(part * count, (part + 1) * count, body, 0)


def place(incoming, base):
    vmem = pl.BlockSpec(memory_space=pltpu.VMEM)
    return pl.pallas_call(
        place_kernel,
        out_shape=jax.ShapeDtypeStruct((SIDE, SIDE), F32),
        in_specs=[pl.BlockSpec(memory_space=pl.ANY), vmem],
        out_specs=vmem,
        scratch_shapes=[
            pltpu.VMEM((64, TILE, TILE), F32),
            pltpu.SMEM((64, TILE), F32),
            pltpu.SemaphoreType.DMA((4,)),
            pltpu.SemaphoreType.DMA,
        ],
        cost_estimate=pl.CostEstimate(flops=COST, bytes_accessed=12 << 20, transcendentals=0),
        name="place",
    )(incoming, base)


def chunk_source(d):
    return divmod(K * TILE + CHUNK * d, PANEL)


def rechunk_pairs():
    first, second, third = [], [], []
    taken = set()
    for d in range(64):
        source, offset = chunk_source(d)
        if source in taken:
            third.append((source, d))
        else:
            taken.add(source)
            first.append((source, d))
        if offset + CHUNK > PANEL:
            second.append((source + 1, d))
    return first, second, third


def across(pairs):
    return [(a * 8 + q, b * 8 + q) for a, b in pairs for q in range(8)]


def program(
    leaf_entries,
    leaf_tiles,
    leaf_map,
    mid_entries,
    mid_tiles,
    mid_map,
    root_panel_entries,
    root_update_entries,
):
    position = lax.axis_index(WIDE)
    row = position // 8
    panel = root_panel_entries[0]
    first, second, third = rechunk_pairs()
    head = lax.ppermute(panel, WIDE, first)
    tail = lax.ppermute(panel, WIDE, second)
    extra = lax.ppermute(panel[CHUNK:], WIDE, third)
    spread = [lax.ppermute(panel, WIDE, across([(0, b)])) for b in (1, 2, 6)]
    leaf_updates = leaves(leaf_entries[0])
    joined = jnp.concatenate([head[:CHUNK], head[CHUNK:] + extra, tail], axis=0)
    offset = (K * TILE + CHUNK * position) % PANEL
    chunk = lax.dynamic_slice_in_dim(joined, offset, CHUNK, 0)
    block = jnp.where(row == 0, panel, 0.0) + (spread[0] + spread[1] + spread[2])
    straight = lax.ppermute(
        chunk, WIDE, [(p * 8 + q, q * 8 + p) for p in range(8) for q in range(8)]
    )
    crossed = lax.ppermute(
        chunk, WIDE, [(p * 8 + q, (q ^ 1) * 8 + p) for p in range(8) for q in range(8)]
    )
    last = lax.ppermute(block, WIDE, across([(1, 3), (2, 4), (6, 7), (0, 5)]))
    outgoing = middles(
        leaf_tiles[0],
        leaf_map[0].reshape(-1),
        mid_tiles[0],
        mid_map[0, 0],
        leaf_updates,
        mid_entries[0, 0],
        chunk,
        block,
    )
    incoming = lax.all_to_all(outgoing, WIDE, 0, 0, tiled=True)
    pair = jnp.where(
        row % 2 == 0,
        jnp.concatenate([straight, crossed], axis=0),
        jnp.concatenate([crossed, straight], axis=0),
    )
    both = lax.all_gather(jnp.concatenate([chunk, block + last], axis=0), ("l", "c"), axis=0)
    cols = lax.all_gather(pair, "y", axis=0, tiled=True)
    rows = both[:, :CHUNK].reshape(SIDE, K * TILE)
    pivot_block = both[:, CHUNK:].reshape(8 * PANEL, K * TILE)[: K * TILE]
    inverse = pivots(pivot_block)
    root_panel, base = updates(
        (position * PANEL).reshape(1), rows, cols, panel, inverse, root_update_entries[0, 0]
    )
    total = place(incoming, base)
    top_part = lax.psum_scatter(total, "grp", scatter_dimension=0, tiled=True)
    return (root_panel[None], top_part[None])


def solution(mesh):
    fine = Mesh(mesh.devices.reshape(4, 4, 2, 4, 2), ("grp",) + WIDE)
    placed = (
        P("grp", WIDE, None, None),
        P("grp", WIDE),
        P("grp", WIDE, None),
        P("grp", WIDE, None, None),
        P("grp", WIDE),
        P("grp", WIDE, None),
        P("grp", WIDE, None),
        P("grp", WIDE, None, None),
    )
    return jax.shard_map(
        program,
        mesh=fine,
        in_specs=placed,
        out_specs=(P("grp", WIDE, None), P(WIDE, "grp", None)),
        check_vma=False,
    )
```

```python
import jax
import jax.numpy as jnp
from jax import lax
from jax.experimental import pallas as pl
from jax.experimental.pallas import tpu as pltpu
from jax.sharding import Mesh, PartitionSpec as P


TILE = 128
UL = 3
UM = 7
K = 4
BLK = 16
SLOT = 136
PANEL = 120
CHUNK = 112
MIXED = PANEL + CHUNK
SIDE = 896
HI = lax.Precision.HIGHEST
F32 = jnp.float32
COST = 1 << 31
WIDE = ("y", "h", "l", "c")


def dot(lhs, rhs, contract):
    return lax.dot_general(
        lhs, rhs, (contract, ((), ())), precision=HI, preferred_element_type=F32
    )


def factor_rows(panels):
    for block in range(TILE // BLK):
        low = block * BLK
        high = low + BLK
        work = []
        for ref, row, col, tiles in panels:
            rows = [
                ref[pl.ds(row + low, BLK), pl.ds(col + t * TILE, TILE)] for t in range(tiles)
            ]
            cols = [
                jnp.broadcast_to(rows[0][:, low + m : low + m + 1], (BLK, TILE))
                for m in range(BLK)
            ]
            work.append((rows, cols))
        for step in range(BLK):
            for (ref, row, col, tiles), (rows, cols) in zip(panels, work):
                inverse = lax.rsqrt(cols[step][step : step + 1, :])
                lower = cols[step] * inverse
                for t in range(tiles):
                    upper = rows[t][step : step + 1, :] * inverse
                    ref[pl.ds(row + low + step, 1), pl.ds(col + t * TILE, TILE)] = upper
                    if step + 1 < BLK:
                        rows[t] = rows[t] - lower * upper
                for m in range(step + 1, BLK):
                    cols[m] = cols[m] - lower * lower[m : m + 1, :]
        if high < TILE:
            for ref, row, col, tiles in panels:
                wide = pl.ds(col, tiles * TILE)
                strip = ref[pl.ds(row + low, BLK), wide]
                product = dot(strip[:, :TILE], strip, ((0,), (0,)))
                rest = pl.ds(row + high, TILE - high)
                ref[rest, wide] = ref[rest, wide] - product[high:]


def leaf_kernel(leaf_ref, out_ref, top):
    for i in range(2):
        top[i * TILE : (i + 1) * TILE, :] = leaf_ref[i, :TILE, :]
    factor_rows([(top, i * TILE, 0, UL + 1) for i in range(2)])
    for i in range(2):
        coupling = top[i * TILE : (i + 1) * TILE, TILE:]
        out_ref[i] = leaf_ref[i, TILE:, TILE:] - dot(coupling, coupling, ((0,), (0,)))


def leaves(leaf):
    return pl.pallas_call(
        leaf_kernel,
        out_shape=jax.ShapeDtypeStruct((2, UL * TILE, UL * TILE), F32),
        scratch_shapes=[pltpu.VMEM((2 * TILE, (UL + 1) * TILE), F32)],
        cost_estimate=pl.CostEstimate(flops=COST, bytes_accessed=3 << 20, transcendentals=0),
        name="leaves",
    )(leaf)


def middle_kernel(
    leaf_live, leaf_map, mid_live, mid_map, leaf_ref, mid_hbm, chunk_hbm, block_hbm, out_hbm,
    mid, update, spots, load_sem, send_sem, spot_sem,
):
    head = pltpu.make_async_copy(mid_hbm.at[:TILE], mid.at[:TILE], load_sem.at[0])
    rest = pltpu.make_async_copy(mid_hbm.at[TILE:], mid.at[TILE:], load_sem.at[1])
    head.start()
    rest.start()

    def assemble(in_head):
        for i in range(2):
            live = leaf_live[i]
            for a in range(UL):
                to_row = leaf_map[i * UL + a]
                row = pl.multiple_of(to_row * TILE, TILE)
                wanted = (to_row == 0) if in_head else (to_row > 0)
                for b in range(UL):
                    col = pl.multiple_of(leaf_map[i * UL + b] * TILE, TILE)

                    @pl.when(wanted & (a < live) & (b < live))
                    def _():
                        mid[pl.ds(row, TILE), pl.ds(col, TILE)] = (
                            mid[pl.ds(row, TILE), pl.ds(col, TILE)]
                            + leaf_ref[i, a * TILE : (a + 1) * TILE, b * TILE : (b + 1) * TILE]
                        )

    head.wait()
    assemble(True)
    factor_rows([(mid, 0, 0, UM + 1)])
    rest.wait()
    assemble(False)
    live = mid_live[0]
    spots[...] = jnp.zeros((64, SLOT - TILE, TILE), F32)
    copies = []
    for a in range(UM):
        update[a * TILE : (a + 1) * TILE, :] = mid[(a + 1) * TILE : (a + 2) * TILE, TILE:] - dot(
            mid[:TILE, (a + 1) * TILE : (a + 2) * TILE], mid[:TILE, TILE:], ((0,), (0,))
        )
        to_row = mid_map[a]
        for b in range(UM):
            to_col = mid_map[b]
            slot = (to_row // 7) * 8 + to_col // 7
            spot = (to_row % 7) * 7 + to_col % 7 + 1
            spot = jnp.where((a < live) & (b < live), spot, 0)
            spots[slot] = jnp.full((SLOT - TILE, TILE), spot.astype(F32), F32)
            copy = pltpu.make_async_copy(
                update.at[a * TILE : (a + 1) * TILE, b * TILE : (b + 1) * TILE],
                out_hbm.at[slot, :TILE, :],
                send_sem.at[a * UM + b],
            )
            copy.start()
            copies.append(copy)
    mark = pltpu.make_async_copy(spots, out_hbm.at[:, TILE:, :], spot_sem)
    mark.start()
    for copy in copies:
        copy.wait()
    mark.wait()


def middles(leaf_live, leaf_map, mid_live, mid_map, leaf, mid, chunk, block):
    smem = pl.BlockSpec(memory_space=pltpu.SMEM)
    vmem = pl.BlockSpec(memory_space=pltpu.VMEM)
    hbm = pl.BlockSpec(memory_space=pl.ANY)
    return pl.pallas_call(
        middle_kernel,
        out_shape=jax.ShapeDtypeStruct((64, SLOT, TILE), F32),
        in_specs=[smem, smem, smem, smem, vmem, hbm, hbm, hbm],
        out_specs=hbm,
        scratch_shapes=[
            pltpu.VMEM((1024, 1024), F32),
            pltpu.VMEM((SIDE, SIDE), F32),
            pltpu.VMEM((64, SLOT - TILE, TILE), F32),
            pltpu.SemaphoreType.DMA((2,)),
            pltpu.SemaphoreType.DMA((UM * UM,)),
            pltpu.SemaphoreType.DMA,
        ],
        cost_estimate=pl.CostEstimate(flops=COST, bytes_accessed=9 << 20, transcendentals=0),
        name="middles",
    )(leaf_live, leaf_map, mid_live, mid_map, leaf, mid, chunk, block)


def pivot_kernel(place_at, pieces_ref, inverse_ref, work, panel):
    width = K * TILE
    eye = (
        lax.broadcasted_iota(jnp.int32, (width, width), 0)
        == lax.broadcasted_iota(jnp.int32, (width, width), 1)
    ).astype(F32)
    work[:, width:] = eye
    for piece in range(8):
        at = place_at[piece]
        part = pieces_ref[piece * MIXED + CHUNK : (piece + 1) * MIXED, :]

        @pl.when(at < K)
        def _():
            work[pl.ds(pl.multiple_of(at * PANEL, 8), PANEL), :width] = part

        @pl.when(at == K)
        def _():
            work[K * PANEL : width, :width] = part[: width - K * PANEL]

    def step(k, carry):
        base = pl.multiple_of(k * TILE, TILE)
        cols = pl.ds(base, (K + 1) * TILE)
        panel[...] = work[pl.ds(base, TILE), cols]
        factor_rows([(panel, 0, 0, K + 1)])
        work[pl.ds(base, TILE), cols] = panel[...]
        for m in range(1, K):

            @pl.when(m > k)
            def _():
                rows = slice(m * TILE, (m + 1) * TILE)
                work[rows, cols] = work[rows, cols] - dot(
                    work[pl.ds(base, TILE), rows], panel[...], ((0,), (0,))
                )

        return carry

    lax.fori_loop(0, K, step, 0)
    inverse_ref[...] = work[:, width:]


def pivots(place_at, pieces):
    width = K * TILE
    vmem = pl.BlockSpec(memory_space=pltpu.VMEM)
    return pl.pallas_call(
        pivot_kernel,
        out_shape=jax.ShapeDtypeStruct((width, width), F32),
        in_specs=[pl.BlockSpec(memory_space=pltpu.SMEM), vmem],
        out_specs=vmem,
        scratch_shapes=[
            pltpu.VMEM((width, 2 * width), F32),
            pltpu.VMEM((TILE, (K + 1) * TILE), F32),
        ],
        cost_estimate=pl.CostEstimate(flops=2 * COST, bytes_accessed=2 << 20, transcendentals=0),
        name="pivots",
    )(place_at, pieces)


def split(value):
    high = value.astype(jnp.bfloat16)
    return high, (value - high.astype(F32)).astype(jnp.bfloat16)


def update_kernel(
    first, place_at, quarter_at, pieces_ref, own_ref, inverse_ref, entry_ref, *rest
):
    quarter_refs, (panel_ref, out_ref, raw, high, low) = rest[:4], rest[4:]
    width = K * TILE
    inverse = inverse_ref[...]
    rows_at = first[0] + lax.broadcasted_iota(jnp.int32, (PANEL, width), 0)
    column = lax.broadcasted_iota(jnp.int32, (PANEL, width), 1)
    live = (column <= rows_at) | (rows_at >= width)
    panel_ref[...] = jnp.where(live, dot(own_ref[...], inverse, ((1,), (1,))), 0.0)
    for piece in range(8):
        raw[0, pl.ds(pl.multiple_of(place_at[piece] * CHUNK, 8), CHUNK), :] = pieces_ref[
            piece * MIXED : piece * MIXED + CHUNK, :
        ]
    for piece, ref in enumerate(quarter_refs):
        at = pl.multiple_of(quarter_at[piece] * 2 * CHUNK, 8)
        raw[1, pl.ds(at, 2 * CHUNK), :] = ref[...]
    for side in range(2):
        high[side], low[side] = split(dot(raw[side], inverse, ((1,), (1,))))

    def product(lhs, rhs):
        return lax.dot_general(
            lhs, rhs, (((1,), (1,)), ((), ())), preferred_element_type=F32
        )

    for t in range(7):
        at = slice(t * TILE, (t + 1) * TILE)
        out_ref[at, :] = entry_ref[at, :] - (
            product(high[0, at, :], high[1])
            + (product(high[0, at, :], low[1]) + product(low[0, at, :], high[1]))
        )


def updates(first, place_at, quarter_at, pieces, own, inverse, entries, quarters):
    vmem = pl.BlockSpec(memory_space=pltpu.VMEM)
    return pl.pallas_call(
        update_kernel,
        out_shape=(
            jax.ShapeDtypeStruct((PANEL, K * TILE), F32),
            jax.ShapeDtypeStruct((SIDE, SIDE), F32),
        ),
        in_specs=[pl.BlockSpec(memory_space=pltpu.SMEM)] * 3 + [vmem] * 8,
        out_specs=(vmem, vmem),
        scratch_shapes=[
            pltpu.VMEM((2, SIDE, K * TILE), F32),
            pltpu.VMEM((2, SIDE, K * TILE), jnp.bfloat16),
            pltpu.VMEM((2, SIDE, K * TILE), jnp.bfloat16),
        ],
        cost_estimate=pl.CostEstimate(flops=COST, bytes_accessed=12 << 20, transcendentals=0),
        name="updates",
    )(first, place_at, quarter_at, pieces, own, inverse, entries, *quarters)


def place_kernel(incoming_hbm, base_ref, out_ref, incoming, spots, sem, spot_sem):
    parts = 4
    count = 64 // parts
    mark = pltpu.make_async_copy(incoming_hbm.at[:, TILE, :], spots, spot_sem)
    mark.start()
    copies = []
    for part in range(parts):
        at = pl.ds(part * count, count)
        copy = pltpu.make_async_copy(
            incoming_hbm.at[at, :TILE, :], incoming.at[at], sem.at[part]
        )
        copy.start()
        copies.append(copy)
    out_ref[...] = base_ref[...]
    mark.wait()
    for part, copy in enumerate(copies):
        copy.wait()

        def body(s, carry):
            spot = spots[s, 0].astype(jnp.int32)

            @pl.when(spot > 0)
            def _():
                row = pl.multiple_of(((spot - 1) // 7) * TILE, TILE)
                col = pl.multiple_of(((spot - 1) % 7) * TILE, TILE)
                out_ref[pl.ds(row, TILE), pl.ds(col, TILE)] = (
                    out_ref[pl.ds(row, TILE), pl.ds(col, TILE)] + incoming[s]
                )

            return carry

        lax.fori_loop(part * count, (part + 1) * count, body, 0)


def place(incoming, base):
    vmem = pl.BlockSpec(memory_space=pltpu.VMEM)
    return pl.pallas_call(
        place_kernel,
        out_shape=jax.ShapeDtypeStruct((SIDE, SIDE), F32),
        in_specs=[pl.BlockSpec(memory_space=pl.ANY), vmem],
        out_specs=vmem,
        scratch_shapes=[
            pltpu.VMEM((64, TILE, TILE), F32),
            pltpu.SMEM((64, TILE), F32),
            pltpu.SemaphoreType.DMA((4,)),
            pltpu.SemaphoreType.DMA,
        ],
        cost_estimate=pl.CostEstimate(flops=COST, bytes_accessed=12 << 20, transcendentals=0),
        name="place",
    )(incoming, base)


def chunk_source(d):
    return divmod(K * TILE + CHUNK * d, PANEL)


def rechunk_pairs():
    first, second, third = [], [], []
    taken = set()
    for d in range(64):
        source, offset = chunk_source(d)
        if source in taken:
            third.append((source, d))
        else:
            taken.add(source)
            first.append((source, d))
        if offset + CHUNK > PANEL:
            second.append((source + 1, d))
    return first, second, third


def across(pairs):
    return [(a * 8 + q, b * 8 + q) for a, b in pairs for q in range(8)]


def program(
    leaf_entries,
    leaf_tiles,
    leaf_map,
    mid_entries,
    mid_tiles,
    mid_map,
    root_panel_entries,
    root_update_entries,
):
    position = lax.axis_index(WIDE)
    row = position // 8
    panel = root_panel_entries[0]
    first, second, third = rechunk_pairs()
    head = lax.ppermute(panel, WIDE, first)
    tail = lax.ppermute(panel, WIDE, second)
    extra = lax.ppermute(panel[CHUNK:], WIDE, third)
    spread = [lax.ppermute(panel, WIDE, across([(0, b)])) for b in (1, 2, 6)]
    leaf_updates = leaves(leaf_entries[0])
    joined = jnp.concatenate([head[:CHUNK], head[CHUNK:] + extra, tail], axis=0)
    offset = (K * TILE + CHUNK * position) % PANEL
    chunk = lax.dynamic_slice_in_dim(joined, offset, CHUNK, 0)
    block = jnp.where(row == 0, panel, 0.0) + (spread[0] + spread[1] + spread[2])
    straight = lax.ppermute(
        chunk, WIDE, [(p * 8 + q, q * 8 + p) for p in range(8) for q in range(8)]
    )
    crossed = lax.ppermute(
        chunk, WIDE, [(p * 8 + q, (q ^ 1) * 8 + p) for p in range(8) for q in range(8)]
    )
    last = lax.ppermute(block, WIDE, across([(1, 3), (2, 4), (6, 7), (0, 5)]))
    outgoing = middles(
        leaf_tiles[0],
        leaf_map[0].reshape(-1),
        mid_tiles[0],
        mid_map[0, 0],
        leaf_updates,
        mid_entries[0, 0],
        chunk,
        block,
    )
    pair = jnp.where(
        row % 2 == 0,
        jnp.concatenate([straight, crossed], axis=0),
        jnp.concatenate([crossed, straight], axis=0),
    )
    mixed = jnp.concatenate([chunk, block + last], axis=0)
    parts = [mixed] + [
        lax.ppermute(mixed, WIDE, [(d, d ^ (2 * k)) for d in range(64)]) for k in (1, 2, 3)
    ]
    quarters = [pair] + [
        lax.ppermute(pair, WIDE, [(d, d ^ (16 * k)) for d in range(64)]) for k in (1, 2, 3)
    ]
    incoming = lax.all_to_all(outgoing, WIDE, 0, 0, tiled=True)
    pieces = lax.all_gather(jnp.concatenate(parts, axis=0), "c", axis=0, tiled=True)
    order = jnp.arange(4, dtype=jnp.int32)
    line = lax.axis_index("l") ^ order
    place_at = jnp.concatenate([2 * line, 2 * line + 1])
    inverse = pivots(place_at, pieces)
    root_panel, base = updates(
        (position * PANEL).reshape(1),
        place_at,
        lax.axis_index("y") ^ order,
        pieces,
        panel,
        inverse,
        root_update_entries[0, 0],
        quarters,
    )
    total = place(incoming, base)
    top_part = lax.psum_scatter(total, "grp", scatter_dimension=0, tiled=True)
    return (root_panel[None], top_part[None])


def solution(mesh):
    fine = Mesh(mesh.devices.reshape(4, 4, 2, 4, 2), ("grp",) + WIDE)
    placed = (
        P("grp", WIDE, None, None),
        P("grp", WIDE),
        P("grp", WIDE, None),
        P("grp", WIDE, None, None),
        P("grp", WIDE),
        P("grp", WIDE, None),
        P("grp", WIDE, None),
        P("grp", WIDE, None, None),
    )
    return jax.shard_map(
        program,
        mesh=fine,
        in_specs=placed,
        out_specs=(P("grp", WIDE, None), P(WIDE, "grp", None)),
        check_vma=False,
    )
```

```python
import jax
import jax.numpy as jnp
from jax import lax
from jax.experimental import pallas as pl
from jax.experimental.pallas import tpu as pltpu
from jax.sharding import Mesh, PartitionSpec as P


TILE = 128
UL = 3
UM = 7
K = 4
BLK = 16
SLOT = 136
PANEL = 120
CHUNK = 112
SIDE = 896
HI = lax.Precision.HIGHEST
F32 = jnp.float32
COST = 1 << 31
WIDE = ("y", "h", "l", "c")


def dot(lhs, rhs, contract):
    return lax.dot_general(
        lhs, rhs, (contract, ((), ())), precision=HI, preferred_element_type=F32
    )


def factor_rows(panels):
    for block in range(TILE // BLK):
        low = block * BLK
        high = low + BLK
        work = []
        for ref, row, col, tiles in panels:
            rows = [
                ref[pl.ds(row + low, BLK), pl.ds(col + t * TILE, TILE)] for t in range(tiles)
            ]
            cols = [
                jnp.broadcast_to(rows[0][:, low + m : low + m + 1], (BLK, TILE))
                for m in range(BLK)
            ]
            work.append((rows, cols))
        for step in range(BLK):
            for (ref, row, col, tiles), (rows, cols) in zip(panels, work):
                inverse = lax.rsqrt(cols[step][step : step + 1, :])
                lower = cols[step] * inverse
                for t in range(tiles):
                    upper = rows[t][step : step + 1, :] * inverse
                    ref[pl.ds(row + low + step, 1), pl.ds(col + t * TILE, TILE)] = upper
                    if step + 1 < BLK:
                        rows[t] = rows[t] - lower * upper
                for m in range(step + 1, BLK):
                    cols[m] = cols[m] - lower * lower[m : m + 1, :]
        if high < TILE:
            for ref, row, col, tiles in panels:
                wide = pl.ds(col, tiles * TILE)
                strip = ref[pl.ds(row + low, BLK), wide]
                product = dot(strip[:, :TILE], strip, ((0,), (0,)))
                rest = pl.ds(row + high, TILE - high)
                ref[rest, wide] = ref[rest, wide] - product[high:]


def leaf_kernel(leaf_ref, out_ref, top):
    for i in range(2):
        top[i * TILE : (i + 1) * TILE, :] = leaf_ref[i, :TILE, :]
    factor_rows([(top, i * TILE, 0, UL + 1) for i in range(2)])
    for i in range(2):
        coupling = top[i * TILE : (i + 1) * TILE, TILE:]
        out_ref[i] = leaf_ref[i, TILE:, TILE:] - dot(coupling, coupling, ((0,), (0,)))


def leaves(leaf):
    return pl.pallas_call(
        leaf_kernel,
        out_shape=jax.ShapeDtypeStruct((2, UL * TILE, UL * TILE), F32),
        scratch_shapes=[pltpu.VMEM((2 * TILE, (UL + 1) * TILE), F32)],
        cost_estimate=pl.CostEstimate(flops=COST, bytes_accessed=3 << 20, transcendentals=0),
        name="leaves",
    )(leaf)


def middle_kernel(
    leaf_live, leaf_map, mid_live, mid_map, leaf_ref, mid_hbm, out_hbm,
    mid, update, spots, load_sem, send_sem, spot_sem,
):
    head = pltpu.make_async_copy(mid_hbm.at[:TILE], mid.at[:TILE], load_sem.at[0])
    rest = pltpu.make_async_copy(mid_hbm.at[TILE:], mid.at[TILE:], load_sem.at[1])
    head.start()
    rest.start()

    def assemble(in_head):
        for i in range(2):
            live = leaf_live[i]
            for a in range(UL):
                to_row = leaf_map[i * UL + a]
                row = pl.multiple_of(to_row * TILE, TILE)
                wanted = (to_row == 0) if in_head else (to_row > 0)
                for b in range(UL):
                    col = pl.multiple_of(leaf_map[i * UL + b] * TILE, TILE)

                    @pl.when(wanted & (a < live) & (b < live))
                    def _():
                        mid[pl.ds(row, TILE), pl.ds(col, TILE)] = (
                            mid[pl.ds(row, TILE), pl.ds(col, TILE)]
                            + leaf_ref[i, a * TILE : (a + 1) * TILE, b * TILE : (b + 1) * TILE]
                        )

    head.wait()
    assemble(True)
    factor_rows([(mid, 0, 0, UM + 1)])
    rest.wait()
    assemble(False)
    live = mid_live[0]
    spots[...] = jnp.zeros((64, SLOT - TILE, TILE), F32)
    copies = []
    for a in range(UM):
        update[a * TILE : (a + 1) * TILE, :] = mid[(a + 1) * TILE : (a + 2) * TILE, TILE:] - dot(
            mid[:TILE, (a + 1) * TILE : (a + 2) * TILE], mid[:TILE, TILE:], ((0,), (0,))
        )
        to_row = mid_map[a]
        for b in range(UM):
            to_col = mid_map[b]
            slot = (to_row // 7) * 8 + to_col // 7
            spot = (to_row % 7) * 7 + to_col % 7 + 1
            spot = jnp.where((a < live) & (b < live), spot, 0)
            spots[slot] = jnp.full((SLOT - TILE, TILE), spot.astype(F32), F32)
            copy = pltpu.make_async_copy(
                update.at[a * TILE : (a + 1) * TILE, b * TILE : (b + 1) * TILE],
                out_hbm.at[slot, :TILE, :],
                send_sem.at[a * UM + b],
            )
            copy.start()
            copies.append(copy)
    mark = pltpu.make_async_copy(spots, out_hbm.at[:, TILE:, :], spot_sem)
    mark.start()
    for copy in copies:
        copy.wait()
    mark.wait()


def middles(leaf_live, leaf_map, mid_live, mid_map, leaf, mid):
    smem = pl.BlockSpec(memory_space=pltpu.SMEM)
    vmem = pl.BlockSpec(memory_space=pltpu.VMEM)
    hbm = pl.BlockSpec(memory_space=pl.ANY)
    return pl.pallas_call(
        middle_kernel,
        out_shape=jax.ShapeDtypeStruct((64, SLOT, TILE), F32),
        in_specs=[smem, smem, smem, smem, vmem, hbm],
        out_specs=hbm,
        scratch_shapes=[
            pltpu.VMEM((1024, 1024), F32),
            pltpu.VMEM((SIDE, SIDE), F32),
            pltpu.VMEM((64, SLOT - TILE, TILE), F32),
            pltpu.SemaphoreType.DMA((2,)),
            pltpu.SemaphoreType.DMA((UM * UM,)),
            pltpu.SemaphoreType.DMA,
        ],
        cost_estimate=pl.CostEstimate(flops=COST, bytes_accessed=9 << 20, transcendentals=0),
        name="middles",
    )(leaf_live, leaf_map, mid_live, mid_map, leaf, mid)


def pivot_kernel(place_at, pieces_ref, inverse_ref, work, panel):
    width = K * TILE
    eye = (
        lax.broadcasted_iota(jnp.int32, (width, width), 0)
        == lax.broadcasted_iota(jnp.int32, (width, width), 1)
    ).astype(F32)
    work[:, width:] = eye
    for piece in range(8):
        at = place_at[piece]
        part = pieces_ref[piece * PANEL : (piece + 1) * PANEL, :]

        @pl.when(at < K)
        def _():
            work[pl.ds(pl.multiple_of(at * PANEL, 8), PANEL), :width] = part

        @pl.when(at == K)
        def _():
            work[K * PANEL : width, :width] = part[: width - K * PANEL]

    def step(k, carry):
        base = pl.multiple_of(k * TILE, TILE)
        cols = pl.ds(base, (K + 1) * TILE)
        panel[...] = work[pl.ds(base, TILE), cols]
        factor_rows([(panel, 0, 0, K + 1)])
        work[pl.ds(base, TILE), cols] = panel[...]
        for m in range(1, K):

            @pl.when(m > k)
            def _():
                rows = slice(m * TILE, (m + 1) * TILE)
                work[rows, cols] = work[rows, cols] - dot(
                    work[pl.ds(base, TILE), rows], panel[...], ((0,), (0,))
                )

        return carry

    lax.fori_loop(0, K, step, 0)
    inverse_ref[...] = work[:, width:]


def pivots(place_at, pieces):
    width = K * TILE
    vmem = pl.BlockSpec(memory_space=pltpu.VMEM)
    return pl.pallas_call(
        pivot_kernel,
        out_shape=jax.ShapeDtypeStruct((width, width), F32),
        in_specs=[pl.BlockSpec(memory_space=pltpu.SMEM), vmem],
        out_specs=vmem,
        scratch_shapes=[
            pltpu.VMEM((width, 2 * width), F32),
            pltpu.VMEM((TILE, (K + 1) * TILE), F32),
        ],
        cost_estimate=pl.CostEstimate(flops=2 * COST, bytes_accessed=2 << 20, transcendentals=0),
        name="pivots",
    )(place_at, pieces)


def split(value):
    high = value.astype(jnp.bfloat16)
    return high, (value - high.astype(F32)).astype(jnp.bfloat16)


def update_kernel(
    first, place_at, quarter_at, inverse_ref, own_ref, pieces_hbm, entry_hbm, *rest
):
    quarter_hbms, rest = rest[:4], rest[4:]
    panel_ref, out_hbm, raw, total, high, low, load_sem, entry_sem, store_sem = rest
    width = K * TILE
    loads = [[], []]
    for piece, hbm in enumerate(quarter_hbms):
        at = pl.multiple_of(quarter_at[piece] * 2 * CHUNK, 8)
        loads[1].append(
            pltpu.make_async_copy(
                hbm, raw.at[1, pl.ds(at, 2 * CHUNK), :], load_sem.at[1, piece]
            )
        )
    for piece in range(8):
        at = pl.multiple_of(place_at[piece] * CHUNK, 8)
        loads[0].append(
            pltpu.make_async_copy(
                pieces_hbm.at[piece * CHUNK : (piece + 1) * CHUNK, :],
                raw.at[0, pl.ds(at, CHUNK), :],
                load_sem.at[0, piece],
            )
        )
    entries = pltpu.make_async_copy(entry_hbm, total, entry_sem)
    for copy in loads[1] + loads[0] + [entries]:
        copy.start()
    inverse = inverse_ref[...]
    rows_at = first[0] + lax.broadcasted_iota(jnp.int32, (PANEL, width), 0)
    column = lax.broadcasted_iota(jnp.int32, (PANEL, width), 1)
    live = (column <= rows_at) | (rows_at >= width)
    panel_ref[...] = jnp.where(live, dot(own_ref[...], inverse, ((1,), (1,))), 0.0)
    for side in (1, 0):
        for copy in loads[side]:
            copy.wait()
        high[side], low[side] = split(dot(raw[side], inverse, ((1,), (1,))))
    entries.wait()

    def product(lhs, rhs):
        return lax.dot_general(
            lhs, rhs, (((1,), (1,)), ((), ())), preferred_element_type=F32
        )

    stores = []
    for t in range(7):
        at = slice(t * TILE, (t + 1) * TILE)
        total[at, :] = total[at, :] - (
            product(high[0, at, :], high[1])
            + (product(high[0, at, :], low[1]) + product(low[0, at, :], high[1]))
        )
        copy = pltpu.make_async_copy(total.at[at, :], out_hbm.at[at, :], store_sem.at[t])
        copy.start()
        stores.append(copy)
    for copy in stores:
        copy.wait()


def updates(first, place_at, quarter_at, inverse, own, pieces, entries, quarters):
    smem = pl.BlockSpec(memory_space=pltpu.SMEM)
    vmem = pl.BlockSpec(memory_space=pltpu.VMEM)
    hbm = pl.BlockSpec(memory_space=pl.ANY)
    return pl.pallas_call(
        update_kernel,
        out_shape=(
            jax.ShapeDtypeStruct((PANEL, K * TILE), F32),
            jax.ShapeDtypeStruct((SIDE, SIDE), F32),
        ),
        in_specs=[smem] * 3 + [vmem] * 2 + [hbm] * 6,
        out_specs=(vmem, hbm),
        scratch_shapes=[
            pltpu.VMEM((2, SIDE, K * TILE), F32),
            pltpu.VMEM((SIDE, SIDE), F32),
            pltpu.VMEM((2, SIDE, K * TILE), jnp.bfloat16),
            pltpu.VMEM((2, SIDE, K * TILE), jnp.bfloat16),
            pltpu.SemaphoreType.DMA((2, 8)),
            pltpu.SemaphoreType.DMA,
            pltpu.SemaphoreType.DMA((7,)),
        ],
        cost_estimate=pl.CostEstimate(flops=COST, bytes_accessed=12 << 20, transcendentals=0),
        name="updates",
    )(first, place_at, quarter_at, inverse, own, pieces, entries, *quarters)


def place_kernel(
    incoming_hbm, base_hbm, out_hbm, incoming, total, spots, sem, base_sem, store_sem, spot_sem
):
    parts = 4
    count = 64 // parts
    mark = pltpu.make_async_copy(incoming_hbm.at[:, TILE, :], spots, spot_sem)
    mark.start()
    base = pltpu.make_async_copy(base_hbm, total, base_sem)
    base.start()
    copies = []
    for piece in range(parts):
        at = pl.ds(piece * count, count)
        copy = pltpu.make_async_copy(
            incoming_hbm.at[at, :TILE, :], incoming.at[at], sem.at[piece]
        )
        copy.start()
        copies.append(copy)
    mark.wait()
    base.wait()
    for piece, copy in enumerate(copies):
        copy.wait()

        def body(s, carry):
            spot = spots[s, 0].astype(jnp.int32)

            @pl.when(spot > 0)
            def _():
                row = pl.multiple_of(((spot - 1) // 7) * TILE, TILE)
                col = pl.multiple_of(((spot - 1) % 7) * TILE, TILE)
                total[pl.ds(row, TILE), pl.ds(col, TILE)] = (
                    total[pl.ds(row, TILE), pl.ds(col, TILE)] + incoming[s]
                )

            return carry

        lax.fori_loop(piece * count, (piece + 1) * count, body, 0)
    store = pltpu.make_async_copy(total, out_hbm, store_sem)
    store.start()
    store.wait()


def place(incoming, base):
    hbm = pl.BlockSpec(memory_space=pl.ANY)
    return pl.pallas_call(
        place_kernel,
        out_shape=jax.ShapeDtypeStruct((SIDE, SIDE), F32),
        in_specs=[hbm, hbm],
        out_specs=hbm,
        scratch_shapes=[
            pltpu.VMEM((64, TILE, TILE), F32),
            pltpu.VMEM((SIDE, SIDE), F32),
            pltpu.SMEM((64, TILE), F32),
            pltpu.SemaphoreType.DMA((4,)),
            pltpu.SemaphoreType.DMA,
            pltpu.SemaphoreType.DMA,
            pltpu.SemaphoreType.DMA,
        ],
        cost_estimate=pl.CostEstimate(flops=COST // 4, bytes_accessed=10 << 20, transcendentals=0),
        name="place",
    )(incoming, base)


def chunk_source(d):
    return divmod(K * TILE + CHUNK * d, PANEL)


def rechunk_pairs():
    first, second, third = [], [], []
    taken = set()
    for d in range(64):
        source, offset = chunk_source(d)
        if source in taken:
            third.append((source, d))
        else:
            taken.add(source)
            first.append((source, d))
        if offset + CHUNK > PANEL:
            second.append((source + 1, d))
    return first, second, third


def across(pairs):
    return [(a * 8 + q, b * 8 + q) for a, b in pairs for q in range(8)]


def program(
    leaf_entries,
    leaf_tiles,
    leaf_map,
    mid_entries,
    mid_tiles,
    mid_map,
    root_panel_entries,
    root_update_entries,
):
    position = lax.axis_index(WIDE)
    row = position // 8
    panel = root_panel_entries[0]
    first, second, third = rechunk_pairs()
    head = lax.ppermute(panel, WIDE, first)
    tail = lax.ppermute(panel, WIDE, second)
    extra = lax.ppermute(panel[CHUNK:], WIDE, third)
    spread = [lax.ppermute(panel, WIDE, across([(0, b)])) for b in (1, 2, 6)]
    leaf_updates = leaves(leaf_entries[0])
    joined = jnp.concatenate([head[:CHUNK], head[CHUNK:] + extra, tail], axis=0)
    offset = (K * TILE + CHUNK * position) % PANEL
    chunk = lax.dynamic_slice_in_dim(joined, offset, CHUNK, 0)
    block = jnp.where(row == 0, panel, 0.0) + (spread[0] + spread[1] + spread[2])
    straight = lax.ppermute(
        chunk, WIDE, [(p * 8 + q, q * 8 + p) for p in range(8) for q in range(8)]
    )
    crossed = lax.ppermute(
        chunk, WIDE, [(p * 8 + q, (q ^ 1) * 8 + p) for p in range(8) for q in range(8)]
    )
    last = lax.ppermute(block, WIDE, across([(1, 3), (2, 4), (6, 7), (0, 5)]))
    outgoing = middles(
        leaf_tiles[0],
        leaf_map[0].reshape(-1),
        mid_tiles[0],
        mid_map[0, 0],
        leaf_updates,
        mid_entries[0, 0],
    )
    pair = jnp.where(
        row % 2 == 0,
        jnp.concatenate([straight, crossed], axis=0),
        jnp.concatenate([crossed, straight], axis=0),
    )
    mixed = jnp.concatenate([chunk, block + last], axis=0)
    parts = [mixed] + [
        lax.ppermute(mixed, WIDE, [(d, d ^ (2 * k)) for d in range(64)]) for k in (1, 2, 3)
    ]
    quarters = [pair] + [
        lax.ppermute(pair, WIDE, [(d, d ^ (16 * k)) for d in range(64)]) for k in (1, 2, 3)
    ]
    incoming = lax.all_to_all(outgoing, WIDE, 0, 0, tiled=True)
    pivot_parts = jnp.concatenate([part[CHUNK:] for part in parts], axis=0)
    chunk_parts = jnp.concatenate([part[:CHUNK] for part in parts], axis=0)
    pivot_pieces = lax.all_gather(pivot_parts, "c", axis=0, tiled=True)
    pieces = lax.all_gather(chunk_parts, "c", axis=0, tiled=True)
    order = jnp.arange(4, dtype=jnp.int32)
    line = lax.axis_index("l") ^ order
    place_at = jnp.concatenate([2 * line, 2 * line + 1])
    inverse = pivots(place_at, pivot_pieces)
    root_panel, base = updates(
        (position * PANEL).reshape(1),
        place_at,
        lax.axis_index("y") ^ order,
        inverse,
        panel,
        pieces,
        root_update_entries[0, 0],
        quarters,
    )
    total = place(incoming, base)
    top_part = lax.psum_scatter(total, "grp", scatter_dimension=0, tiled=True)
    return (root_panel[None], top_part[None])


def solution(mesh):
    fine = Mesh(mesh.devices.reshape(4, 4, 2, 4, 2), ("grp",) + WIDE)
    placed = (
        P("grp", WIDE, None, None),
        P("grp", WIDE),
        P("grp", WIDE, None),
        P("grp", WIDE, None, None),
        P("grp", WIDE),
        P("grp", WIDE, None),
        P("grp", WIDE, None),
        P("grp", WIDE, None, None),
    )
    return jax.shard_map(
        program,
        mesh=fine,
        in_specs=placed,
        out_specs=(P("grp", WIDE, None), P(WIDE, "grp", None)),
        check_vma=False,
    )
```

```python
import jax
import jax.numpy as jnp
from jax import lax
from jax.experimental import pallas as pl
from jax.experimental.pallas import tpu as pltpu
from jax.sharding import Mesh, PartitionSpec as P


TILE = 128
UL = 3
UM = 7
K = 4
BLK = 16
SLOT = 136
HOLDERS = 5
PANEL = 120
CHUNK = 112
SIDE = 896
HI = lax.Precision.HIGHEST
F32 = jnp.float32
COST = 1 << 31
WIDE = ("y", "h", "l", "c")


def dot(lhs, rhs, contract):
    return lax.dot_general(
        lhs, rhs, (contract, ((), ())), precision=HI, preferred_element_type=F32
    )


def factor_rows(panels):
    for block in range(TILE // BLK):
        low = block * BLK
        high = low + BLK
        work = []
        for ref, row, col, tiles in panels:
            rows = [
                ref[pl.ds(row + low, BLK), pl.ds(col + t * TILE, TILE)] for t in range(tiles)
            ]
            cols = [
                jnp.broadcast_to(rows[0][:, low + m : low + m + 1], (BLK, TILE))
                for m in range(BLK)
            ]
            work.append((rows, cols))
        for step in range(BLK):
            for (ref, row, col, tiles), (rows, cols) in zip(panels, work):
                inverse = lax.rsqrt(cols[step][step : step + 1, :])
                lower = cols[step] * inverse
                for t in range(tiles):
                    upper = rows[t][step : step + 1, :] * inverse
                    ref[pl.ds(row + low + step, 1), pl.ds(col + t * TILE, TILE)] = upper
                    if step + 1 < BLK:
                        rows[t] = rows[t] - lower * upper
                for m in range(step + 1, BLK):
                    cols[m] = cols[m] - lower * lower[m : m + 1, :]
        if high < TILE:
            for ref, row, col, tiles in panels:
                wide = pl.ds(col, tiles * TILE)
                strip = ref[pl.ds(row + low, BLK), wide]
                product = dot(strip[:, :TILE], strip, ((0,), (0,)))
                rest = pl.ds(row + high, TILE - high)
                ref[rest, wide] = ref[rest, wide] - product[high:]


def leaf_kernel(leaf_ref, out_ref, top):
    for i in range(2):
        top[i * TILE : (i + 1) * TILE, :] = leaf_ref[i, :TILE, :]
    factor_rows([(top, i * TILE, 0, UL + 1) for i in range(2)])
    for i in range(2):
        coupling = top[i * TILE : (i + 1) * TILE, TILE:]
        out_ref[i] = leaf_ref[i, TILE:, TILE:] - dot(coupling, coupling, ((0,), (0,)))


def leaves(leaf):
    return pl.pallas_call(
        leaf_kernel,
        out_shape=jax.ShapeDtypeStruct((2, UL * TILE, UL * TILE), F32),
        scratch_shapes=[pltpu.VMEM((2 * TILE, (UL + 1) * TILE), F32)],
        cost_estimate=pl.CostEstimate(flops=COST, bytes_accessed=3 << 20, transcendentals=0),
        name="leaves",
    )(leaf)


def middle_kernel(
    leaf_live, leaf_map, mid_live, mid_map, leaf_ref, mid_hbm, out_hbm,
    mid, update, spots, load_sem, send_sem, spot_sem,
):
    head = pltpu.make_async_copy(mid_hbm.at[:TILE], mid.at[:TILE], load_sem.at[0])
    rest = pltpu.make_async_copy(mid_hbm.at[TILE:], mid.at[TILE:], load_sem.at[1])
    head.start()
    rest.start()

    def assemble(in_head):
        def body(n, carry):
            i = n // (UL * UL)
            a = (n // UL) % UL
            b = n % UL
            to_row = leaf_map[i * UL + a]
            row = pl.multiple_of(to_row * TILE, TILE)
            col = pl.multiple_of(leaf_map[i * UL + b] * TILE, TILE)
            from_row = pl.multiple_of(a * TILE, TILE)
            from_col = pl.multiple_of(b * TILE, TILE)
            wanted = (to_row == 0) if in_head else (to_row > 0)

            @pl.when(wanted & (a < leaf_live[i]) & (b < leaf_live[i]))
            def _():
                mid[pl.ds(row, TILE), pl.ds(col, TILE)] = (
                    mid[pl.ds(row, TILE), pl.ds(col, TILE)]
                    + leaf_ref[i, pl.ds(from_row, TILE), pl.ds(from_col, TILE)]
                )

            return carry

        lax.fori_loop(0, 2 * UL * UL, body, 0)

    head.wait()
    assemble(True)
    factor_rows([(mid, 0, 0, UM + 1)])
    rest.wait()
    assemble(False)
    live = mid_live[0]
    spots[...] = jnp.zeros((64, SLOT - TILE, TILE), F32)
    copies = []
    for a in range(UM):
        update[a * TILE : (a + 1) * TILE, :] = mid[(a + 1) * TILE : (a + 2) * TILE, TILE:] - dot(
            mid[:TILE, (a + 1) * TILE : (a + 2) * TILE], mid[:TILE, TILE:], ((0,), (0,))
        )
        to_row = mid_map[a]
        for b in range(UM):
            to_col = mid_map[b]
            slot = (to_row // 7) * 8 + to_col // 7
            spot = (to_row % 7) * 7 + to_col % 7 + 1
            spot = jnp.where((a < live) & (b < live), spot, 0)
            spots[slot] = jnp.full((SLOT - TILE, TILE), spot.astype(F32), F32)
            copy = pltpu.make_async_copy(
                update.at[a * TILE : (a + 1) * TILE, b * TILE : (b + 1) * TILE],
                out_hbm.at[slot, :TILE, :],
                send_sem.at[a * UM + b],
            )
            copy.start()
            copies.append(copy)
    mark = pltpu.make_async_copy(spots, out_hbm.at[:, TILE:, :], spot_sem)
    mark.start()
    for copy in copies:
        copy.wait()
    mark.wait()


def middles(leaf_live, leaf_map, mid_live, mid_map, leaf, mid):
    smem = pl.BlockSpec(memory_space=pltpu.SMEM)
    vmem = pl.BlockSpec(memory_space=pltpu.VMEM)
    hbm = pl.BlockSpec(memory_space=pl.ANY)
    return pl.pallas_call(
        middle_kernel,
        out_shape=jax.ShapeDtypeStruct((64, SLOT, TILE), F32),
        in_specs=[smem, smem, smem, smem, vmem, hbm],
        out_specs=hbm,
        scratch_shapes=[
            pltpu.VMEM((1024, 1024), F32),
            pltpu.VMEM((SIDE, SIDE), F32),
            pltpu.VMEM((64, SLOT - TILE, TILE), F32),
            pltpu.SemaphoreType.DMA((2,)),
            pltpu.SemaphoreType.DMA((UM * UM,)),
            pltpu.SemaphoreType.DMA,
        ],
        cost_estimate=pl.CostEstimate(flops=COST, bytes_accessed=9 << 20, transcendentals=0),
        name="middles",
    )(leaf_live, leaf_map, mid_live, mid_map, leaf, mid)


def pivot_kernel(place_at, pieces_ref, inverse_ref, work, panel):
    width = K * TILE
    eye = (
        lax.broadcasted_iota(jnp.int32, (width, width), 0)
        == lax.broadcasted_iota(jnp.int32, (width, width), 1)
    ).astype(F32)
    work[:, width:] = eye
    for piece in range(8):
        at = place_at[piece]
        part = pieces_ref[piece * PANEL : (piece + 1) * PANEL, :]

        @pl.when(at < K)
        def _():
            work[pl.ds(pl.multiple_of(at * PANEL, 8), PANEL), :width] = part

        @pl.when(at == K)
        def _():
            work[K * PANEL : width, :width] = part[: width - K * PANEL]

    def step(k, carry):
        base = pl.multiple_of(k * TILE, TILE)
        cols = pl.ds(base, (K + 1) * TILE)
        panel[...] = work[pl.ds(base, TILE), cols]
        factor_rows([(panel, 0, 0, K + 1)])
        work[pl.ds(base, TILE), cols] = panel[...]
        for m in range(1, K):

            @pl.when(m > k)
            def _():
                rows = slice(m * TILE, (m + 1) * TILE)
                work[rows, cols] = work[rows, cols] - dot(
                    work[pl.ds(base, TILE), rows], panel[...], ((0,), (0,))
                )

        return carry

    lax.fori_loop(0, K, step, 0)
    inverse_ref[...] = work[:, width:]


def pivots(place_at, pieces):
    width = K * TILE
    vmem = pl.BlockSpec(memory_space=pltpu.VMEM)
    return pl.pallas_call(
        pivot_kernel,
        out_shape=jax.ShapeDtypeStruct((width, width), F32),
        in_specs=[pl.BlockSpec(memory_space=pltpu.SMEM), vmem],
        out_specs=vmem,
        scratch_shapes=[
            pltpu.VMEM((width, 2 * width), F32),
            pltpu.VMEM((TILE, (K + 1) * TILE), F32),
        ],
        cost_estimate=pl.CostEstimate(flops=2 * COST, bytes_accessed=2 << 20, transcendentals=0),
        name="pivots",
    )(place_at, pieces)


def split(value):
    high = value.astype(jnp.bfloat16)
    return high, (value - high.astype(F32)).astype(jnp.bfloat16)


def update_kernel(
    first, inverse_ref, own_ref, rows_hbm, cols_hbm, entry_hbm, panel_ref, out_hbm,
    raw, total, high, low, load_sem, entry_sem, store_sem,
):
    width = K * TILE
    loads = [
        pltpu.make_async_copy(hbm, raw.at[side], load_sem.at[side])
        for side, hbm in enumerate((rows_hbm, cols_hbm))
    ]
    entries = pltpu.make_async_copy(entry_hbm, total, entry_sem)
    for copy in loads + [entries]:
        copy.start()
    inverse = inverse_ref[...]
    rows_at = first[0] + lax.broadcasted_iota(jnp.int32, (PANEL, width), 0)
    column = lax.broadcasted_iota(jnp.int32, (PANEL, width), 1)
    live = (column <= rows_at) | (rows_at >= width)
    panel_ref[...] = jnp.where(live, dot(own_ref[...], inverse, ((1,), (1,))), 0.0)
    for side in range(2):
        loads[side].wait()
        high[side], low[side] = split(dot(raw[side], inverse, ((1,), (1,))))
    entries.wait()

    def product(lhs, rhs):
        return lax.dot_general(
            lhs, rhs, (((1,), (1,)), ((), ())), preferred_element_type=F32
        )

    stores = []
    for t in range(7):
        at = slice(t * TILE, (t + 1) * TILE)
        total[at, :] = total[at, :] - (
            product(high[0, at, :], high[1])
            + (product(high[0, at, :], low[1]) + product(low[0, at, :], high[1]))
        )
        copy = pltpu.make_async_copy(total.at[at, :], out_hbm.at[at, :], store_sem.at[t])
        copy.start()
        stores.append(copy)
    for copy in stores:
        copy.wait()


def updates(first, inverse, own, rows, cols, entries):
    smem = pl.BlockSpec(memory_space=pltpu.SMEM)
    vmem = pl.BlockSpec(memory_space=pltpu.VMEM)
    hbm = pl.BlockSpec(memory_space=pl.ANY)
    return pl.pallas_call(
        update_kernel,
        out_shape=(
            jax.ShapeDtypeStruct((PANEL, K * TILE), F32),
            jax.ShapeDtypeStruct((SIDE, SIDE), F32),
        ),
        in_specs=[smem] + [vmem] * 2 + [hbm] * 3,
        out_specs=(vmem, hbm),
        scratch_shapes=[
            pltpu.VMEM((2, SIDE, K * TILE), F32),
            pltpu.VMEM((SIDE, SIDE), F32),
            pltpu.VMEM((2, SIDE, K * TILE), jnp.bfloat16),
            pltpu.VMEM((2, SIDE, K * TILE), jnp.bfloat16),
            pltpu.SemaphoreType.DMA((2,)),
            pltpu.SemaphoreType.DMA,
            pltpu.SemaphoreType.DMA((7,)),
        ],
        cost_estimate=pl.CostEstimate(flops=COST, bytes_accessed=12 << 20, transcendentals=0),
        name="updates",
    )(first, inverse, own, rows, cols, entries)


def place_kernel(
    incoming_hbm, base_hbm, out_hbm, incoming, total, spots, sem, base_sem, store_sem, spot_sem
):
    parts = 4
    count = 64 // parts
    mark = pltpu.make_async_copy(incoming_hbm.at[:, TILE, :], spots, spot_sem)
    mark.start()
    base = pltpu.make_async_copy(base_hbm, total, base_sem)
    base.start()
    copies = []
    for piece in range(parts):
        at = pl.ds(piece * count, count)
        copy = pltpu.make_async_copy(
            incoming_hbm.at[at, :TILE, :], incoming.at[at], sem.at[piece]
        )
        copy.start()
        copies.append(copy)
    mark.wait()
    base.wait()
    for piece, copy in enumerate(copies):
        copy.wait()

        def body(s, carry):
            spot = spots[s, 0].astype(jnp.int32)

            @pl.when(spot > 0)
            def _():
                row = pl.multiple_of(((spot - 1) // 7) * TILE, TILE)
                col = pl.multiple_of(((spot - 1) % 7) * TILE, TILE)
                total[pl.ds(row, TILE), pl.ds(col, TILE)] = (
                    total[pl.ds(row, TILE), pl.ds(col, TILE)] + incoming[s]
                )

            return carry

        lax.fori_loop(piece * count, (piece + 1) * count, body, 0)
    store = pltpu.make_async_copy(total, out_hbm, store_sem)
    store.start()
    store.wait()


def place(incoming, base):
    hbm = pl.BlockSpec(memory_space=pl.ANY)
    return pl.pallas_call(
        place_kernel,
        out_shape=jax.ShapeDtypeStruct((SIDE, SIDE), F32),
        in_specs=[hbm, hbm],
        out_specs=hbm,
        scratch_shapes=[
            pltpu.VMEM((64, TILE, TILE), F32),
            pltpu.VMEM((SIDE, SIDE), F32),
            pltpu.SMEM((64, TILE), F32),
            pltpu.SemaphoreType.DMA((4,)),
            pltpu.SemaphoreType.DMA,
            pltpu.SemaphoreType.DMA,
            pltpu.SemaphoreType.DMA,
        ],
        cost_estimate=pl.CostEstimate(flops=COST // 4, bytes_accessed=10 << 20, transcendentals=0),
        name="place",
    )(incoming, base)


def chunk_source(d):
    return divmod(K * TILE + CHUNK * d, PANEL)


def rechunk_pairs():
    first, second, third = [], [], []
    taken = set()
    for d in range(64):
        source, offset = chunk_source(d)
        if source in taken:
            third.append((source, d))
        else:
            taken.add(source)
            first.append((source, d))
        if offset + CHUNK > PANEL:
            second.append((source + 1, d))
    return first, second, third


def across(pairs):
    return [(a * 8 + q, b * 8 + q) for a, b in pairs for q in range(HOLDERS)]


def program(
    leaf_entries,
    leaf_tiles,
    leaf_map,
    mid_entries,
    mid_tiles,
    mid_map,
    root_panel_entries,
    root_update_entries,
):
    position = lax.axis_index(WIDE)
    row = position // 8
    panel = root_panel_entries[0]
    first, second, third = rechunk_pairs()
    head = lax.ppermute(panel, WIDE, first)
    tail = lax.ppermute(panel, WIDE, second)
    extra = lax.ppermute(panel[CHUNK:], WIDE, third)
    spread = [lax.ppermute(panel, WIDE, across([(0, b)])) for b in (1, 2, 6)]
    leaf_updates = leaves(leaf_entries[0])
    joined = jnp.concatenate([head[:CHUNK], head[CHUNK:] + extra, tail], axis=0)
    offset = (K * TILE + CHUNK * position) % PANEL
    chunk = lax.dynamic_slice_in_dim(joined, offset, CHUNK, 0)
    block = jnp.where(row == 0, panel, 0.0) + (spread[0] + spread[1] + spread[2])
    straight = lax.ppermute(
        chunk, WIDE, [(p * 8 + q, q * 8 + p) for p in range(8) for q in range(8)]
    )
    crossed = lax.ppermute(
        chunk, WIDE, [(p * 8 + q, (q ^ 1) * 8 + p) for p in range(8) for q in range(8)]
    )
    last = lax.ppermute(block, WIDE, across([(1, 3), (2, 4), (6, 7), (0, 5)]))
    outgoing = middles(
        leaf_tiles[0],
        leaf_map[0].reshape(-1),
        mid_tiles[0],
        mid_map[0, 0],
        leaf_updates,
        mid_entries[0, 0],
    )
    pair = jnp.where(
        row % 2 == 0,
        jnp.concatenate([straight, crossed], axis=0),
        jnp.concatenate([crossed, straight], axis=0),
    )
    block = block + last
    parts = [block] + [
        lax.ppermute(
            block, WIDE, [(d, d ^ (2 * k)) for d in range(64) if d % 8 < HOLDERS]
        )
        for k in (1, 2, 3)
    ]
    incoming = lax.all_to_all(outgoing, WIDE, 0, 0, tiled=True)
    rows = lax.all_gather(chunk, ("l", "c"), axis=0, tiled=True)
    pivot_pieces = lax.all_gather(jnp.concatenate(parts, axis=0), "c", axis=0, tiled=True)
    cols = lax.all_gather(pair, "y", axis=0, tiled=True)
    order = jnp.arange(4, dtype=jnp.int32)
    line = lax.axis_index("l") ^ order
    place_at = jnp.concatenate([2 * line, 2 * line + 1])
    inverse = pivots(place_at, pivot_pieces)
    root_panel, base = updates(
        (position * PANEL).reshape(1),
        inverse,
        panel,
        rows,
        cols,
        root_update_entries[0, 0],
    )
    total = place(incoming, base)
    top_part = lax.psum_scatter(total, "grp", scatter_dimension=0, tiled=True)
    return (root_panel[None], top_part[None])


def solution(mesh):
    fine = Mesh(mesh.devices.reshape(4, 4, 2, 4, 2), ("grp",) + WIDE)
    placed = (
        P("grp", WIDE, None, None),
        P("grp", WIDE),
        P("grp", WIDE, None),
        P("grp", WIDE, None, None),
        P("grp", WIDE),
        P("grp", WIDE, None),
        P("grp", WIDE, None),
        P("grp", WIDE, None, None),
    )
    return jax.shard_map(
        program,
        mesh=fine,
        in_specs=placed,
        out_specs=(P("grp", WIDE, None), P(WIDE, "grp", None)),
        check_vma=False,
    )
```

```python
import jax
import jax.numpy as jnp
from jax import lax
from jax.experimental import pallas as pl
from jax.experimental.pallas import tpu as pltpu
from jax.sharding import Mesh, PartitionSpec as P


TILE = 128
UL = 3
UM = 7
K = 4
BLK = 16
SLOT = 136
HOLDERS = 5
PANEL = 120
CHUNK = 112
SIDE = 896
HI = lax.Precision.HIGHEST
F32 = jnp.float32
COST = 1 << 31
WIDE = ("y", "h", "l", "c")


def dot(lhs, rhs, contract):
    return lax.dot_general(
        lhs, rhs, (contract, ((), ())), precision=HI, preferred_element_type=F32
    )


def factor_rows(panels):
    for block in range(TILE // BLK):
        low = block * BLK
        high = low + BLK
        work = []
        for ref, row, col, tiles in panels:
            rows = [
                ref[pl.ds(row + low, BLK), pl.ds(col + t * TILE, TILE)] for t in range(tiles)
            ]
            cols = [
                jnp.broadcast_to(rows[0][:, low + m : low + m + 1], (BLK, TILE))
                for m in range(BLK)
            ]
            work.append((rows, cols))
        for step in range(BLK):
            for (ref, row, col, tiles), (rows, cols) in zip(panels, work):
                inverse = lax.rsqrt(cols[step][step : step + 1, :])
                lower = cols[step] * inverse
                for t in range(tiles):
                    upper = rows[t][step : step + 1, :] * inverse
                    ref[pl.ds(row + low + step, 1), pl.ds(col + t * TILE, TILE)] = upper
                    if step + 1 < BLK:
                        rows[t] = rows[t] - lower * upper
                for m in range(step + 1, BLK):
                    cols[m] = cols[m] - lower * lower[m : m + 1, :]
        if high < TILE:
            for ref, row, col, tiles in panels:
                wide = pl.ds(col, tiles * TILE)
                strip = ref[pl.ds(row + low, BLK), wide]
                product = dot(strip[:, :TILE], strip, ((0,), (0,)))
                rest = pl.ds(row + high, TILE - high)
                ref[rest, wide] = ref[rest, wide] - product[high:]


def leaf_kernel(leaf_ref, out_ref, top):
    for i in range(2):
        top[i * TILE : (i + 1) * TILE, :] = leaf_ref[i, :TILE, :]
    factor_rows([(top, i * TILE, 0, UL + 1) for i in range(2)])
    for i in range(2):
        coupling = top[i * TILE : (i + 1) * TILE, TILE:]
        out_ref[i] = leaf_ref[i, TILE:, TILE:] - dot(coupling, coupling, ((0,), (0,)))


def leaves(leaf):
    return pl.pallas_call(
        leaf_kernel,
        out_shape=jax.ShapeDtypeStruct((2, UL * TILE, UL * TILE), F32),
        scratch_shapes=[pltpu.VMEM((2 * TILE, (UL + 1) * TILE), F32)],
        cost_estimate=pl.CostEstimate(flops=COST, bytes_accessed=3 << 20, transcendentals=0),
        name="leaves",
    )(leaf)


def middle_kernel(
    leaf_live, leaf_map, mid_live, mid_map, leaf_ref, mid_hbm, out_hbm,
    mid, update, spots, load_sem, send_sem, spot_sem,
):
    head = pltpu.make_async_copy(mid_hbm.at[:TILE], mid.at[:TILE], load_sem.at[0])
    rest = pltpu.make_async_copy(mid_hbm.at[TILE:], mid.at[TILE:], load_sem.at[1])
    head.start()
    rest.start()

    def assemble(in_head):
        def body(n, carry):
            i = n // (UL * UL)
            a = (n // UL) % UL
            b = n % UL
            to_row = leaf_map[i * UL + a]
            row = pl.multiple_of(to_row * TILE, TILE)
            col = pl.multiple_of(leaf_map[i * UL + b] * TILE, TILE)
            from_row = pl.multiple_of(a * TILE, TILE)
            from_col = pl.multiple_of(b * TILE, TILE)
            wanted = (to_row == 0) if in_head else (to_row > 0)

            @pl.when(wanted & (a < leaf_live[i]) & (b < leaf_live[i]))
            def _():
                mid[pl.ds(row, TILE), pl.ds(col, TILE)] = (
                    mid[pl.ds(row, TILE), pl.ds(col, TILE)]
                    + leaf_ref[i, pl.ds(from_row, TILE), pl.ds(from_col, TILE)]
                )

            return carry

        lax.fori_loop(0, 2 * UL * UL, body, 0)

    head.wait()
    assemble(True)
    factor_rows([(mid, 0, 0, UM + 1)])
    rest.wait()
    assemble(False)
    live = mid_live[0]
    spots[...] = jnp.zeros((64, SLOT - TILE, TILE), F32)
    copies = []
    for a in range(UM):
        update[a * TILE : (a + 1) * TILE, :] = mid[(a + 1) * TILE : (a + 2) * TILE, TILE:] - dot(
            mid[:TILE, (a + 1) * TILE : (a + 2) * TILE], mid[:TILE, TILE:], ((0,), (0,))
        )
        to_row = mid_map[a]
        for b in range(UM):
            to_col = mid_map[b]
            slot = (to_row // 7) * 8 + to_col // 7
            spot = (to_row % 7) * 7 + to_col % 7 + 1
            spot = jnp.where((a < live) & (b < live), spot, 0)
            spots[slot] = jnp.full((SLOT - TILE, TILE), spot.astype(F32), F32)
            copy = pltpu.make_async_copy(
                update.at[a * TILE : (a + 1) * TILE, b * TILE : (b + 1) * TILE],
                out_hbm.at[slot, :TILE, :],
                send_sem.at[a * UM + b],
            )
            copy.start()
            copies.append(copy)
    mark = pltpu.make_async_copy(spots, out_hbm.at[:, TILE:, :], spot_sem)
    mark.start()
    for copy in copies:
        copy.wait()
    mark.wait()


def middles(leaf_live, leaf_map, mid_live, mid_map, leaf, mid):
    smem = pl.BlockSpec(memory_space=pltpu.SMEM)
    vmem = pl.BlockSpec(memory_space=pltpu.VMEM)
    hbm = pl.BlockSpec(memory_space=pl.ANY)
    return pl.pallas_call(
        middle_kernel,
        out_shape=jax.ShapeDtypeStruct((64, SLOT, TILE), F32),
        in_specs=[smem, smem, smem, smem, vmem, hbm],
        out_specs=hbm,
        scratch_shapes=[
            pltpu.VMEM((1024, 1024), F32),
            pltpu.VMEM((SIDE, SIDE), F32),
            pltpu.VMEM((64, SLOT - TILE, TILE), F32),
            pltpu.SemaphoreType.DMA((2,)),
            pltpu.SemaphoreType.DMA((UM * UM,)),
            pltpu.SemaphoreType.DMA,
        ],
        cost_estimate=pl.CostEstimate(flops=COST, bytes_accessed=9 << 20, transcendentals=0),
        name="middles",
    )(leaf_live, leaf_map, mid_live, mid_map, leaf, mid)


def pivot_kernel(pieces_ref, inverse_ref, work, panel):
    width = K * TILE
    eye = (
        lax.broadcasted_iota(jnp.int32, (width, width), 0)
        == lax.broadcasted_iota(jnp.int32, (width, width), 1)
    ).astype(F32)
    work[:, width:] = eye
    work[:, :width] = pieces_ref[:width, :]

    def step(k, carry):
        base = pl.multiple_of(k * TILE, TILE)
        cols = pl.ds(base, (K + 1) * TILE)
        panel[...] = work[pl.ds(base, TILE), cols]
        factor_rows([(panel, 0, 0, K + 1)])
        work[pl.ds(base, TILE), cols] = panel[...]
        for m in range(1, K):

            @pl.when(m > k)
            def _():
                rows = slice(m * TILE, (m + 1) * TILE)
                work[rows, cols] = work[rows, cols] - dot(
                    work[pl.ds(base, TILE), rows], panel[...], ((0,), (0,))
                )

        return carry

    lax.fori_loop(0, K, step, 0)
    inverse_ref[...] = work[:, width:]


def pivots(pieces):
    width = K * TILE
    vmem = pl.BlockSpec(memory_space=pltpu.VMEM)
    return pl.pallas_call(
        pivot_kernel,
        out_shape=jax.ShapeDtypeStruct((width, width), F32),
        in_specs=[vmem],
        out_specs=vmem,
        scratch_shapes=[
            pltpu.VMEM((width, 2 * width), F32),
            pltpu.VMEM((TILE, (K + 1) * TILE), F32),
        ],
        cost_estimate=pl.CostEstimate(flops=2 * COST, bytes_accessed=2 << 20, transcendentals=0),
        name="pivots",
    )(pieces)


def split(value):
    high = value.astype(jnp.bfloat16)
    return high, (value - high.astype(F32)).astype(jnp.bfloat16)


def update_kernel(
    first, quarter_at, inverse_ref, own_ref, rows_hbm, entry_hbm, *rest
):
    quarter_hbms, rest = rest[:4], rest[4:]
    panel_ref, out_hbm, raw, total, high, low, load_sem, entry_sem, store_sem = rest
    width = K * TILE
    loads = [[pltpu.make_async_copy(rows_hbm, raw.at[0], load_sem.at[0])], []]
    for piece, hbm in enumerate(quarter_hbms):
        at = pl.multiple_of(quarter_at[piece] * 2 * CHUNK, 8)
        loads[1].append(
            pltpu.make_async_copy(
                hbm, raw.at[1, pl.ds(at, 2 * CHUNK), :], load_sem.at[1 + piece]
            )
        )
    entries = pltpu.make_async_copy(entry_hbm, total, entry_sem)
    for copy in loads[0] + loads[1] + [entries]:
        copy.start()
    inverse = inverse_ref[...]
    rows_at = first[0] + lax.broadcasted_iota(jnp.int32, (PANEL, width), 0)
    column = lax.broadcasted_iota(jnp.int32, (PANEL, width), 1)
    live = (column <= rows_at) | (rows_at >= width)
    panel_ref[...] = jnp.where(live, dot(own_ref[...], inverse, ((1,), (1,))), 0.0)
    for side in range(2):
        for copy in loads[side]:
            copy.wait()
        high[side], low[side] = split(dot(raw[side], inverse, ((1,), (1,))))
    entries.wait()

    def product(lhs, rhs):
        return lax.dot_general(
            lhs, rhs, (((1,), (1,)), ((), ())), preferred_element_type=F32
        )

    stores = []
    for t in range(7):
        at = slice(t * TILE, (t + 1) * TILE)
        total[at, :] = total[at, :] - (
            product(high[0, at, :], high[1])
            + (product(high[0, at, :], low[1]) + product(low[0, at, :], high[1]))
        )
        copy = pltpu.make_async_copy(total.at[at, :], out_hbm.at[at, :], store_sem.at[t])
        copy.start()
        stores.append(copy)
    for copy in stores:
        copy.wait()


def updates(first, quarter_at, inverse, own, rows, entries, quarters):
    smem = pl.BlockSpec(memory_space=pltpu.SMEM)
    vmem = pl.BlockSpec(memory_space=pltpu.VMEM)
    hbm = pl.BlockSpec(memory_space=pl.ANY)
    return pl.pallas_call(
        update_kernel,
        out_shape=(
            jax.ShapeDtypeStruct((PANEL, K * TILE), F32),
            jax.ShapeDtypeStruct((SIDE, SIDE), F32),
        ),
        in_specs=[smem] * 2 + [vmem] * 2 + [hbm] * 6,
        out_specs=(vmem, hbm),
        scratch_shapes=[
            pltpu.VMEM((2, SIDE, K * TILE), F32),
            pltpu.VMEM((SIDE, SIDE), F32),
            pltpu.VMEM((2, SIDE, K * TILE), jnp.bfloat16),
            pltpu.VMEM((2, SIDE, K * TILE), jnp.bfloat16),
            pltpu.SemaphoreType.DMA((5,)),
            pltpu.SemaphoreType.DMA,
            pltpu.SemaphoreType.DMA((7,)),
        ],
        cost_estimate=pl.CostEstimate(flops=COST, bytes_accessed=12 << 20, transcendentals=0),
        name="updates",
    )(first, quarter_at, inverse, own, rows, entries, *quarters)


def place_kernel(
    incoming_hbm, base_hbm, out_hbm, incoming, total, spots, sem, base_sem, store_sem, spot_sem
):
    parts = 4
    count = 64 // parts
    mark = pltpu.make_async_copy(incoming_hbm.at[:, TILE, :], spots, spot_sem)
    mark.start()
    base = pltpu.make_async_copy(base_hbm, total, base_sem)
    base.start()
    copies = []
    for piece in range(parts):
        at = pl.ds(piece * count, count)
        copy = pltpu.make_async_copy(
            incoming_hbm.at[at, :TILE, :], incoming.at[at], sem.at[piece]
        )
        copy.start()
        copies.append(copy)
    mark.wait()
    base.wait()
    for piece, copy in enumerate(copies):
        copy.wait()

        def body(s, carry):
            spot = spots[s, 0].astype(jnp.int32)

            @pl.when(spot > 0)
            def _():
                row = pl.multiple_of(((spot - 1) // 7) * TILE, TILE)
                col = pl.multiple_of(((spot - 1) % 7) * TILE, TILE)
                total[pl.ds(row, TILE), pl.ds(col, TILE)] = (
                    total[pl.ds(row, TILE), pl.ds(col, TILE)] + incoming[s]
                )

            return carry

        lax.fori_loop(piece * count, (piece + 1) * count, body, 0)
    store = pltpu.make_async_copy(total, out_hbm, store_sem)
    store.start()
    store.wait()


def place(incoming, base):
    hbm = pl.BlockSpec(memory_space=pl.ANY)
    return pl.pallas_call(
        place_kernel,
        out_shape=jax.ShapeDtypeStruct((SIDE, SIDE), F32),
        in_specs=[hbm, hbm],
        out_specs=hbm,
        scratch_shapes=[
            pltpu.VMEM((64, TILE, TILE), F32),
            pltpu.VMEM((SIDE, SIDE), F32),
            pltpu.SMEM((64, TILE), F32),
            pltpu.SemaphoreType.DMA((4,)),
            pltpu.SemaphoreType.DMA,
            pltpu.SemaphoreType.DMA,
            pltpu.SemaphoreType.DMA,
        ],
        cost_estimate=pl.CostEstimate(flops=COST // 4, bytes_accessed=10 << 20, transcendentals=0),
        name="place",
    )(incoming, base)


def chunk_source(d):
    return divmod(K * TILE + CHUNK * d, PANEL)


def rechunk_pairs():
    first, second, third = [], [], []
    taken = set()
    for d in range(64):
        source, offset = chunk_source(d)
        if source in taken:
            third.append((source, d))
        else:
            taken.add(source)
            first.append((source, d))
        if offset + CHUNK > PANEL:
            second.append((source + 1, d))
    return first, second, third


def program(
    leaf_entries,
    leaf_tiles,
    leaf_map,
    mid_entries,
    mid_tiles,
    mid_map,
    root_panel_entries,
    root_update_entries,
):
    position = lax.axis_index(WIDE)
    row = position // 8
    panel = root_panel_entries[0]
    first, second, third = rechunk_pairs()
    crossing = lax.ppermute(panel, WIDE, [(q, 8 + q) for q in range(HOLDERS)])
    head = lax.ppermute(panel, WIDE, first)
    tail = lax.ppermute(panel, WIDE, second)
    extra = lax.ppermute(panel[CHUNK:], WIDE, third)
    leaf_updates = leaves(leaf_entries[0])
    joined = jnp.concatenate([head[:CHUNK], head[CHUNK:] + extra, tail], axis=0)
    offset = (K * TILE + CHUNK * position) % PANEL
    chunk = lax.dynamic_slice_in_dim(joined, offset, CHUNK, 0)
    block = jnp.where(row % 2 == 0, panel, crossing)
    block = lax.all_gather(
        jnp.concatenate([block, jnp.zeros((16, K * TILE), F32)], axis=0), "y", axis=0
    )[0, :PANEL]
    pivot_pieces = lax.all_gather(block, ("l", "c"), axis=0, tiled=True)
    straight = lax.ppermute(
        chunk, WIDE, [(p * 8 + q, q * 8 + p) for p in range(8) for q in range(8)]
    )
    crossed = lax.ppermute(
        chunk, WIDE, [(p * 8 + q, (q ^ 1) * 8 + p) for p in range(8) for q in range(8)]
    )
    outgoing = middles(
        leaf_tiles[0],
        leaf_map[0].reshape(-1),
        mid_tiles[0],
        mid_map[0, 0],
        leaf_updates,
        mid_entries[0, 0],
    )
    pair = jnp.where(
        row % 2 == 0,
        jnp.concatenate([straight, crossed], axis=0),
        jnp.concatenate([crossed, straight], axis=0),
    )
    quarters = [pair] + [
        lax.ppermute(pair, WIDE, [(d, d ^ (16 * k)) for d in range(64)]) for k in (1, 2, 3)
    ]
    incoming = lax.all_to_all(outgoing, WIDE, 0, 0, tiled=True)
    rows = lax.all_gather(chunk, ("l", "c"), axis=0, tiled=True)
    inverse = pivots(pivot_pieces)
    root_panel, base = updates(
        (position * PANEL).reshape(1),
        lax.axis_index("y") ^ jnp.arange(4, dtype=jnp.int32),
        inverse,
        panel,
        rows,
        root_update_entries[0, 0],
        quarters,
    )
    total = place(incoming, base)
    top_part = lax.psum_scatter(total, "grp", scatter_dimension=0, tiled=True)
    return (root_panel[None], top_part[None])


def solution(mesh):
    fine = Mesh(mesh.devices.reshape(4, 4, 2, 4, 2), ("grp",) + WIDE)
    placed = (
        P("grp", WIDE, None, None),
        P("grp", WIDE),
        P("grp", WIDE, None),
        P("grp", WIDE, None, None),
        P("grp", WIDE),
        P("grp", WIDE, None),
        P("grp", WIDE, None),
        P("grp", WIDE, None, None),
    )
    return jax.shard_map(
        program,
        mesh=fine,
        in_specs=placed,
        out_specs=(P("grp", WIDE, None), P(WIDE, "grp", None)),
        check_vma=False,
    )
```
